32 devices in a mesh: blk: 16 (over z, y, core), head: 2 (over x).
Axes of the slice: x: 2, y: 2, z: 4, core: 2. Of those that a mesh axis runs over, the one named last changes fastest.
Arguments:
- query: bfloat16 [4096, 4096], P(('blk', 'head')), may hold values from -6 to 6
- key: bfloat16 [4096, 1024], P(('blk', 'head')), may hold values from -6 to 6
- value: bfloat16 [4096, 1024], P(('blk', 'head')), may hold values from -6 to 6
- grad_out: bfloat16 [4096, 4096], P(('blk', 'head')), may hold values from -6 to 6
- doc_lengths: int32 [32], replicated, may hold values from 1 to 256, 4096 in all
Outputs:
- attended: bfloat16 [4096, 4096], P(('blk', 'head'))
- grad_query: bfloat16 [4096, 4096], P(('blk', 'head'))
- grad_key: bfloat16 [4096, 1024], P(('blk', 'head'))
- grad_value: bfloat16 [4096, 1024], P(('blk', 'head'))
The draws below stay inside these ranges and needn't reach their ends.
Inputs may be any that keep to these rules, and one draw needn't show every extreme that they name: `doc_lengths`: every document has at most 256 tokens, one has exactly 256, and the lengths sum to 4096.
All inputs are finite; a program needn't handle non-finite values.
Results may differ from the reference program's by a relative error of at most 0.0088.
Values may be sent and summed in bfloat16 or wider, within the bound.
A program may use at most 128 MiB of HBM per device.

```python
import math
import jax
import jax.numpy as jnp
import numpy as np
from jax import lax

HEADS = 32
KV_HEADS = 8
HEAD_DIM = 128
BLOCK = 256
SEQ = 4096
DOC_MOST = 256
DOCS = 32


def draw_query(key, part):
    entry_key = jax.random.fold_in(key, 11)
    result = jnp.clip(jax.random.normal(entry_key, (SEQ, HEADS * HEAD_DIM), jnp.float32), -4.0, 4.0)
    return result.astype(jnp.bfloat16)


def draw_key(key, part):
    entry_key = jax.random.fold_in(key, 12)
    result = jnp.clip(jax.random.normal(entry_key, (SEQ, KV_HEADS * HEAD_DIM), jnp.float32), -4.0, 4.0)
    return result.astype(jnp.bfloat16)


def levels(own_key, dims, shards, low, high):
    factor_of, own = 1.0, jax.random.fold_in(own_key, 6)
    for axis_at, parts in shards:
        heights = jnp.exp(jax.random.uniform(jax.random.fold_in(own, axis_at), (parts,), jnp.float32, low / len(shards), high / len(shards)))
        factor_of = factor_of * jnp.repeat(heights, dims[axis_at] // parts).reshape([-1 if axis == axis_at else 1 for axis in range(len(dims))])
    return factor_of


def split_up(amount, total, limit, lean):
    loads = [(1 << 20) // math.isqrt(rank ** lean) + 1 for rank in range(2, amount + 1)]
    surplus, holding = total - limit - (amount - 1), [1] * (amount - 1)
    while surplus > 0:
        movable = [i for i in range(amount - 1) if holding[i] < limit]
        mass, budget = sum([loads[i] for i in movable]), surplus
        for i in movable:
            extra = min(limit - holding[i], max(1, budget * loads[i] // mass), surplus)
            holding[i] = holding[i] + extra
            surplus = surplus - extra
    return np.array([limit] + holding)


def uneven_parts(stream_key, amount, total, reach, lean):
    if amount == 2:
        one = jax.random.randint(stream_key, (), max(1, total - reach), min(reach, total - 1) + 1)
        return jnp.stack([one, total - one])
    tallies = jnp.asarray(split_up(amount, total, reach, lean), jnp.int32)
    couples = (amount - 1) // 2
    source_of, sink = tallies[1:1 + 2 * couples:2], tallies[2:2 + 2 * couples:2]
    margin = jnp.minimum(source_of - 1, reach - sink)
    moved = jax.random.randint(jax.random.fold_in(stream_key, 1), (couples,), 0, 1 << 20) % (margin + 1)
    tallies = tallies.at[1:1 + 2 * couples:2].set(source_of - moved).at[2:2 + 2 * couples:2].set(sink + moved)
    return tallies[jax.random.permutation(jax.random.fold_in(stream_key, 2), amount)]


def gaussian(key, extent, scale, most, split=(), kind=jnp.bfloat16):
    loudness = levels(key, extent, split, -0.22, 0.18) if split else 1.0
    values = jax.random.normal(key, extent, jnp.float32) * scale * loudness
    return jnp.minimum(jnp.maximum(values, -most), most).astype(kind)


def setup_inputs(seed: int = 0) -> dict:
    keys = jax.random.split(jax.random.key(seed), 6)
    query = draw_query(jax.random.fold_in(keys[5], 71), 0)
    key = draw_key(jax.random.fold_in(keys[5], 71), 0)
    value = gaussian(keys[2], (SEQ, KV_HEADS * HEAD_DIM), 1.0, 6.0, ((0, 32),))
    grad_out = gaussian(keys[3], (SEQ, HEADS * HEAD_DIM), 1.0, 6.0, ((0, 32),))
    doc_lengths = uneven_parts(keys[4], DOCS, SEQ, DOC_MOST, 2).astype(jnp.int32)
    return {"query": query, "key": key, "value": value, "grad_out": grad_out, "doc_lengths": doc_lengths}


def segment_ids(positions, doc_starts):
    return jnp.sum((doc_starts[None, :] <= positions[:, None]).astype(jnp.int32), axis=1) - 1


def reference(query, key, value, grad_out, doc_lengths):
    scaling = HEAD_DIM ** -0.5
    groups = HEADS // KV_HEADS
    row_step = min(512, BLOCK)
    span_rows = DOC_MOST + row_step
    doc_ends = jnp.cumsum(doc_lengths).astype(jnp.int32)
    doc_starts = (doc_ends - doc_lengths).astype(jnp.int32)
    padding = jnp.zeros((DOC_MOST, KV_HEADS * HEAD_DIM), key.dtype)
    keys_padded = jnp.concatenate([padding, key], axis=0)
    values_padded = jnp.concatenate([padding, value], axis=0)
    offsets = jnp.arange(row_step, dtype=jnp.int32)
    reaches = jnp.arange(span_rows, dtype=jnp.int32)

    def visit(carry, tile_number):
        grad_keys, grad_values = carry
        first_row = (tile_number * row_step).astype(jnp.int32)
        query_rows = lax.dynamic_slice_in_dim(query, first_row, row_step, 0).astype(jnp.float32).reshape(row_step, KV_HEADS, groups, HEAD_DIM)
        grad_rows = lax.dynamic_slice_in_dim(grad_out, first_row, row_step, 0).astype(jnp.float32).reshape(row_step, KV_HEADS, groups, HEAD_DIM)
        key_rows = lax.dynamic_slice_in_dim(keys_padded, first_row, span_rows, 0).astype(jnp.float32).reshape(span_rows, KV_HEADS, HEAD_DIM)
        value_rows = lax.dynamic_slice_in_dim(values_padded, first_row, span_rows, 0).astype(jnp.float32).reshape(span_rows, KV_HEADS, HEAD_DIM)
        query_pos = first_row + offsets
        key_pos = first_row - DOC_MOST + reaches
        allowed = (key_pos[None, :] <= query_pos[:, None]) & (segment_ids(query_pos, doc_starts)[:, None] == segment_ids(key_pos, doc_starts)[None, :])
        scores = jnp.einsum('qkgd,skd->kgqs', query_rows, key_rows) * scaling
        scores = jnp.where(allowed[None, None], scores, -jnp.inf)
        peak_score = jnp.max(scores, axis=-1, keepdims=True)
        log_total = peak_score + jnp.log(jnp.sum(jnp.exp(scores - peak_score), axis=-1, keepdims=True))
        weights = jnp.exp(scores - log_total)
        weights_bf = lax.optimization_barrier(weights.astype(jnp.bfloat16)).astype(jnp.float32)
        attended_rows = jnp.einsum('kgqs,skd->qkgd', weights_bf, value_rows).astype(jnp.bfloat16)
        output_rows = lax.optimization_barrier(attended_rows).astype(jnp.float32)
        row_delta = jnp.einsum('qkgd,qkgd->kgq', grad_rows, output_rows)
        grad_weights = jnp.einsum('qkgd,skd->kgqs', grad_rows, value_rows)
        grad_scores = weights * (grad_weights - row_delta[..., None])
        grad_scores = lax.optimization_barrier(grad_scores.astype(jnp.bfloat16)).astype(jnp.float32)
        grad_query_rows = (jnp.einsum('kgqs,skd->qkgd', grad_scores, key_rows) * scaling).astype(jnp.bfloat16)
        key_part = (jnp.einsum('kgqs,qkgd->skd', grad_scores, query_rows) * scaling).reshape(span_rows, KV_HEADS * HEAD_DIM)
        value_part = jnp.einsum('kgqs,qkgd->skd', weights_bf, grad_rows).reshape(span_rows, KV_HEADS * HEAD_DIM)
        current_keys = lax.dynamic_slice_in_dim(grad_keys, first_row, span_rows, 0)
        current_values = lax.dynamic_slice_in_dim(grad_values, first_row, span_rows, 0)
        grad_keys = lax.dynamic_update_slice_in_dim(grad_keys, current_keys + key_part, first_row, 0)
        grad_values = lax.dynamic_update_slice_in_dim(grad_values, current_values + value_part, first_row, 0)
        outputs = (attended_rows.reshape(row_step, HEADS * HEAD_DIM), grad_query_rows.reshape(row_step, HEADS * HEAD_DIM))
        return (grad_keys, grad_values), outputs

    start_keys = jnp.zeros((SEQ + DOC_MOST, KV_HEADS * HEAD_DIM), jnp.float32)
    start_values = jnp.zeros((SEQ + DOC_MOST, KV_HEADS * HEAD_DIM), jnp.float32)
    tile_numbers = jnp.arange(SEQ // row_step, dtype=jnp.int32)
    sums, stacked = lax.scan(visit, (start_keys, start_values), tile_numbers)
    attended = stacked[0].reshape(SEQ, HEADS * HEAD_DIM)
    grad_query = stacked[1].reshape(SEQ, HEADS * HEAD_DIM)
    grad_key = sums[0][DOC_MOST:].astype(jnp.bfloat16)
    grad_value = sums[1][DOC_MOST:].astype(jnp.bfloat16)
    return (attended, grad_query, grad_key, grad_value)
```

```python
import functools
import math

import jax
import jax.numpy as jnp
from jax import lax
from jax.experimental import pallas as pl
from jax.experimental.pallas import tpu as pltpu
from jax.sharding import PartitionSpec as P

HEAD_DIM = 128
EXCLUDED = -1e30
HEADS_A_COPY = 2
MESH = pl.DeviceIdType.MESH


def kernel(
    back, total, lens_hbm, q_hbm, k_hbm, v_hbm, do_hbm, attbuf, dqbuf, dkbuf, dvbuf,
    window, qbuf, dobuf, part, landed, own, bias, lens,
    lens_in, kv_in, q_in, kv_send, kv_recv, g_send, g_recv,
):
    rows = q_hbm.shape[0]
    kv_heads = k_hbm.shape[1] // HEAD_DIM
    groups = q_hbm.shape[1] // k_hbm.shape[1]
    width = groups * HEAD_DIM
    span = (back + 1) * rows
    scaling = HEAD_DIM ** (-0.5)
    chunks = kv_send.shape[1]
    per = kv_heads // chunks
    me = lax.axis_index("blk") * back + lax.axis_index("head")

    def device(number):
        return {"blk": number // back, "head": number % back}

    def columns(g, size):
        return pl.ds(pl.multiple_of(g * size, size), size)

    def heads(c):
        return pl.ds(c * per, per)

    def kv_load(g, which):
        return pltpu.make_async_copy(
            (k_hbm, v_hbm)[which].at[:, columns(g, HEAD_DIM)],
            window.at[0, g, which],
            kv_in.at[which, g],
        )

    def q_load(g, which):
        return pltpu.make_async_copy(
            (q_hbm, do_hbm)[which].at[:, columns(g, width)],
            (qbuf, dobuf)[which].at[g],
            q_in.at[which, g],
        )

    def kv_copy(c, k):
        return pltpu.make_async_remote_copy(
            src_ref=window.at[0, heads(c)],
            dst_ref=window.at[k, heads(c)],
            send_sem=kv_send.at[k - 1, c],
            recv_sem=kv_recv.at[k - 1, c],
            device_id=device(me + k),
            device_id_type=MESH,
        )

    def g_copy(c, k):
        return pltpu.make_async_remote_copy(
            src_ref=part.at[k - 1, heads(c)],
            dst_ref=landed.at[k - 1, heads(c)],
            send_sem=g_send.at[k - 1, c],
            recv_sem=g_recv.at[k - 1, c],
            device_id=device(me - k),
            device_id_type=MESH,
        )

    barrier = pltpu.get_barrier_semaphore()
    for k in range(1, back + 1):
        @pl.when(me - k >= 0)
        def _():
            pl.semaphore_signal(barrier, inc=1, device_id=device(me - k), device_id_type=MESH)

    @pl.loop(0, kv_heads)
    def _(g):
        kv_load(g, 0).start()
        kv_load(g, 1).start()

    lens_load = pltpu.make_async_copy(lens_hbm, lens, lens_in)
    lens_load.start()

    @pl.loop(0, kv_heads)
    def _(g):
        q_load(g, 0).start()
        q_load(g, 1).start()

    @pl.when(me < total - 1)
    def _():
        pl.semaphore_wait(barrier, jnp.minimum(total - 1 - me, back))

    @pl.loop(0, chunks)
    def _(c):
        for i in range(per):
            kv_load(c * per + i, 0).wait()
            kv_load(c * per + i, 1).wait()
        for k in range(1, back + 1):
            @pl.when(me + k < total)
            def _():
                kv_copy(c, k).start()

    for k in range(1, back + 1):
        @pl.when(me - k < 0)
        def _():
            window[k] = jnp.zeros((kv_heads, 2, rows, HEAD_DIM), jnp.bfloat16)

        @pl.when(me + k >= total)
        def _():
            landed[k - 1] = jnp.zeros((kv_heads, 2, rows, HEAD_DIM), jnp.bfloat16)

    lens_load.wait()
    query_pos = me * rows + lax.broadcasted_iota(jnp.int32, (1, rows), 1)

    def latest(d, carry):
        start, first = carry
        return start + lens[d], jnp.where(query_pos >= start, start, first)

    _, first = lax.fori_loop(
        0, lens.shape[0], latest, (jnp.int32(0), jnp.zeros((1, rows), jnp.int32))
    )
    key_pos = (me - back) * rows + lax.broadcasted_iota(jnp.int32, (span, rows), 0)
    bias[...] = jnp.where((key_pos <= query_pos) & (key_pos >= first), 0.0, EXCLUDED)

    def dot(a, b, a_dim, b_dim):
        return lax.dot_general(
            a, b, (((a_dim,), (b_dim,)), ((), ())), preferred_element_type=jnp.float32
        )

    def stacked(values):
        return jnp.concatenate(
            [values[:, h * HEAD_DIM : (h + 1) * HEAD_DIM] for h in range(groups)], axis=0
        )

    @pl.loop(0, kv_heads)
    def _(g):
        q_load(g, 0).wait()
        q_load(g, 1).wait()

        @pl.when(g % per == 0)
        def _():
            for k in range(1, back + 1):
                @pl.when(me - k >= 0)
                def _():
                    kv_copy(g // per, k).wait_recv()

        keys, values = (
            jnp.concatenate([window[k, g, which] for k in range(back, -1, -1)], axis=0)
            for which in range(2)
        )
        queries, grads = stacked(qbuf[g]), stacked(dobuf[g])
        kept = jnp.concatenate([bias[...]] * groups, axis=1)
        scores = dot(keys, queries, 1, 1) * (scaling * math.log2(math.e)) + kept
        peak = jnp.max(scores, axis=0, keepdims=True)
        raised = jnp.exp2(scores - peak)
        weights = raised * (1.0 / jnp.sum(raised, axis=0, keepdims=True))
        weights_bf = weights.astype(jnp.bfloat16)
        attended = dot(values, weights_bf, 0, 0)
        grad_weights = dot(values, grads, 1, 1)
        delta = jnp.sum(weights * grad_weights, axis=0, keepdims=True)
        grad_scores = (weights * (grad_weights - delta)).astype(jnp.bfloat16)
        grad_query = dot(keys, grad_scores, 0, 0) * scaling
        grad_key = dot(grad_scores, queries, 1, 0) * scaling
        grad_value = dot(weights_bf, grads, 1, 0)
        for k in range(1, back + 1):
            at = slice((back - k) * rows, (back - k + 1) * rows)
            part[k - 1, g, 0] = grad_key[at].astype(jnp.bfloat16)
            part[k - 1, g, 1] = grad_value[at].astype(jnp.bfloat16)
        own[g, 0] = grad_key[back * rows :]
        own[g, 1] = grad_value[back * rows :]

        @pl.when(g % per == per - 1)
        def _():
            for k in range(1, back + 1):
                @pl.when(me - k >= 0)
                def _():
                    g_copy(g // per, k).start()

        for h in range(groups):
            at = slice(h * HEAD_DIM, (h + 1) * HEAD_DIM)
            to = columns(g * groups + h, HEAD_DIM)
            attbuf[:, to] = attended[:, at].T.astype(jnp.bfloat16)
            dqbuf[:, to] = grad_query[:, at].T.astype(jnp.bfloat16)

    @pl.loop(0, chunks)
    def _(c):
        for k in range(1, back + 1):
            @pl.when(me + k < total)
            def _():
                g_copy(c, k).wait_recv()
        for i in range(per):
            g = c * per + i
            sums = own[g]
            for k in range(1, back + 1):
                sums = sums + landed[k - 1, g].astype(jnp.float32)
            dkbuf[:, columns(g, HEAD_DIM)] = sums[0].astype(jnp.bfloat16)
            dvbuf[:, columns(g, HEAD_DIM)] = sums[1].astype(jnp.bfloat16)

    @pl.loop(0, chunks)
    def _(c):
        for k in range(1, back + 1):
            @pl.when(me + k < total)
            def _():
                kv_copy(c, k).wait_send()

            @pl.when(me - k >= 0)
            def _():
                g_copy(c, k).wait_send()


def write_out(att, dq, dk, dv, att_hbm, dq_hbm, dk_hbm, dv_hbm, sems):
    pairs = ((att, att_hbm), (dq, dq_hbm), (dk, dk_hbm), (dv, dv_hbm))
    copies = [
        pltpu.make_async_copy(source, target, sems.at[which])
        for which, (source, target) in enumerate(pairs)
    ]
    for copy in copies:
        copy.start()
    for copy in copies:
        copy.wait()


def solution(mesh):
    back = mesh.shape["head"]
    total = mesh.shape["blk"] * back

    def per_device(query, key, value, grad_out, doc_lengths):
        rows, kv_heads = query.shape[0], key.shape[1] // HEAD_DIM
        width = query.shape[1] // kv_heads
        chunks = kv_heads // math.gcd(kv_heads, HEADS_A_COPY)
        bf, f32 = jnp.bfloat16, jnp.float32
        anywhere = pl.BlockSpec(memory_space=pl.ANY)
        dma = pltpu.SemaphoreType.DMA
        results = pl.pallas_call(
            functools.partial(kernel, back, total),
            out_shape=[
                pltpu.VMEM(query.shape, bf),
                pltpu.VMEM(query.shape, bf),
                pltpu.VMEM(key.shape, bf),
                pltpu.VMEM(key.shape, bf),
            ],
            in_specs=[anywhere] * 5,
            out_specs=[pl.BlockSpec(memory_space=pltpu.VMEM)] * 4,
            scratch_shapes=[
                pltpu.VMEM((back + 1, kv_heads, 2, rows, HEAD_DIM), bf),
                pltpu.VMEM((kv_heads, rows, width), bf),
                pltpu.VMEM((kv_heads, rows, width), bf),
                pltpu.VMEM((back, kv_heads, 2, rows, HEAD_DIM), bf),
                pltpu.VMEM((back, kv_heads, 2, rows, HEAD_DIM), bf),
                pltpu.VMEM((kv_heads, 2, rows, HEAD_DIM), f32),
                pltpu.VMEM(((back + 1) * rows, rows), f32),
                pltpu.SMEM(doc_lengths.shape, jnp.int32),
                dma,
                dma((2, kv_heads)),
                dma((2, kv_heads)),
                dma((back, chunks)),
                dma((back, chunks)),
                dma((back, chunks)),
                dma((back, chunks)),
            ],
            compiler_params=pltpu.CompilerParams(collective_id=0, has_side_effects=True),
        )(doc_lengths, query, key, value, grad_out)
        results = [pltpu.with_memory_space_constraint(r, pltpu.VMEM) for r in results]
        return pl.pallas_call(
            write_out,
            out_shape=[
                jax.ShapeDtypeStruct(query.shape, bf),
                jax.ShapeDtypeStruct(query.shape, bf),
                jax.ShapeDtypeStruct(key.shape, bf),
                jax.ShapeDtypeStruct(key.shape, bf),
            ],
            in_specs=[pl.BlockSpec(memory_space=pltpu.VMEM)] * 4,
            out_specs=[anywhere] * 4,
            scratch_shapes=[dma((4,))],
        )(*results)

    split = P(("blk", "head"), None)
    return jax.shard_map(
        per_device,
        mesh=mesh,
        in_specs=(split, split, split, split, P()),
        out_specs=(split, split, split, split),
        check_vma=False,
    )
```

```python
import functools
import math

import jax
import jax.numpy as jnp
from jax import lax
from jax.experimental import pallas as pl
from jax.experimental.pallas import tpu as pltpu
from jax.sharding import PartitionSpec as P

HEAD_DIM = 128
EXCLUDED = -1e30
HEADS_A_COPY = 2
MESH = pl.DeviceIdType.MESH


def kernel(
    back, total, lens_hbm, q_hbm, k_hbm, v_hbm, do_hbm, attbuf, dqbuf, dkbuf, dvbuf,
    window, qbuf, dobuf, part, landed, own, bias, lens,
    lens_in, kv_in, q_in, kv_send, kv_recv, relay_send, g_send, g_recv,
):
    rows = q_hbm.shape[0]
    kv_heads = k_hbm.shape[1] // HEAD_DIM
    groups = q_hbm.shape[1] // k_hbm.shape[1]
    width = groups * HEAD_DIM
    span = (back + 1) * rows
    scaling = HEAD_DIM ** (-0.5)
    chunks = kv_send.shape[1]
    per = kv_heads // chunks
    last = chunks - 1
    me = lax.axis_index("blk") * back + lax.axis_index("head")
    place = me % (2 * back)
    edge = (place == 2 * back - 1) & (me + back < total) & (back == 2)
    relays = (place == 1) & (me > back) & (back == 2)

    def device(number):
        return {"blk": number // back, "head": number % back}

    def columns(g, size):
        return pl.ds(pl.multiple_of(g * size, size), size)

    def heads(c):
        return pl.ds(c * per, per)

    def kv_load(g, which):
        return pltpu.make_async_copy(
            (k_hbm, v_hbm)[which].at[:, columns(g, HEAD_DIM)],
            window.at[0, g, which],
            kv_in.at[which, g],
        )

    def q_load(g, which):
        return pltpu.make_async_copy(
            (q_hbm, do_hbm)[which].at[:, columns(g, width)],
            (qbuf, dobuf)[which].at[g],
            q_in.at[which, g],
        )

    def kv_copy(c, k):
        return pltpu.make_async_remote_copy(
            src_ref=window.at[0, heads(c)],
            dst_ref=window.at[k, heads(c)],
            send_sem=kv_send.at[k - 1, c],
            recv_sem=kv_recv.at[k - 1, c],
            device_id=device(me + k),
            device_id_type=MESH,
        )

    def relay():
        return pltpu.make_async_remote_copy(
            src_ref=window.at[back, heads(last)],
            dst_ref=window.at[1, heads(last)],
            send_sem=relay_send,
            recv_sem=kv_recv.at[0, last],
            device_id=device(me - 1),
            device_id_type=MESH,
        )

    def g_copy(c, k):
        return pltpu.make_async_remote_copy(
            src_ref=part.at[k - 1, heads(c)],
            dst_ref=landed.at[k - 1, heads(c)],
            send_sem=g_send.at[k - 1, c],
            recv_sem=g_recv.at[k - 1, c],
            device_id=device(me - k),
            device_id_type=MESH,
        )

    barrier = pltpu.get_barrier_semaphore()
    for k in range(1, back + 1):
        @pl.when(me - k >= 0)
        def _():
            pl.semaphore_signal(barrier, inc=1, device_id=device(me - k), device_id_type=MESH)

    @pl.loop(0, kv_heads)
    def _(g):
        kv_load(g, 0).start()
        kv_load(g, 1).start()

    lens_load = pltpu.make_async_copy(lens_hbm, lens, lens_in)
    lens_load.start()

    @pl.loop(0, kv_heads)
    def _(g):
        q_load(g, 0).start()
        q_load(g, 1).start()

    @pl.when(me < total - 1)
    def _():
        pl.semaphore_wait(barrier, jnp.minimum(total - 1 - me, back))

    def kv_loaded(c):
        for i in range(per):
            kv_load(c * per + i, 0).wait()
            kv_load(c * per + i, 1).wait()

    @pl.when(edge)
    def _():
        kv_loaded(last)
        kv_copy(last, back).start()

    @pl.loop(0, chunks - edge.astype(jnp.int32))
    def _(c):
        kv_loaded(c)
        for k in range(1, back + 1):
            @pl.when(me + k < total)
            def _():
                kv_copy(c, k).start()

    for k in range(1, back + 1):
        @pl.when(me - k < 0)
        def _():
            window[k] = jnp.zeros((kv_heads, 2, rows, HEAD_DIM), jnp.bfloat16)

        @pl.when(me + k >= total)
        def _():
            landed[k - 1] = jnp.zeros((kv_heads, 2, rows, HEAD_DIM), jnp.bfloat16)

    lens_load.wait()
    query_pos = me * rows + lax.broadcasted_iota(jnp.int32, (1, rows), 1)

    def latest(d, carry):
        start, first = carry
        return start + lens[d], jnp.where(query_pos >= start, start, first)

    _, first = lax.fori_loop(
        0, lens.shape[0], latest, (jnp.int32(0), jnp.zeros((1, rows), jnp.int32))
    )
    key_pos = (me - back) * rows + lax.broadcasted_iota(jnp.int32, (span, rows), 0)
    bias[...] = jnp.where((key_pos <= query_pos) & (key_pos >= first), 0.0, EXCLUDED)

    def dot(a, b, a_dim, b_dim):
        return lax.dot_general(
            a, b, (((a_dim,), (b_dim,)), ((), ())), preferred_element_type=jnp.float32
        )

    def stacked(values):
        return jnp.concatenate(
            [values[:, h * HEAD_DIM : (h + 1) * HEAD_DIM] for h in range(groups)], axis=0
        )

    @pl.loop(0, kv_heads)
    def _(g):
        q_load(g, 0).wait()
        q_load(g, 1).wait()

        @pl.when(g % per == 0)
        def _():
            for k in range(1, back + 1):
                early = relays & (g // per == last) if k == back else False
                @pl.when((me - k >= 0) & jnp.logical_not(early))
                def _():
                    kv_copy(g // per, k).wait_recv()

        @pl.when(relays & (g == 0))
        def _():
            kv_copy(last, back).wait_recv()
            relay().start()

        keys, values = (
            jnp.concatenate([window[k, g, which] for k in range(back, -1, -1)], axis=0)
            for which in range(2)
        )
        queries, grads = stacked(qbuf[g]), stacked(dobuf[g])
        kept = jnp.concatenate([bias[...]] * groups, axis=1)
        scores = dot(keys, queries, 1, 1) * (scaling * math.log2(math.e)) + kept
        peak = jnp.max(scores, axis=0, keepdims=True)
        raised = jnp.exp2(scores - peak)
        weights = raised * (1.0 / jnp.sum(raised, axis=0, keepdims=True))
        weights_bf = weights.astype(jnp.bfloat16)
        attended = dot(values, weights_bf, 0, 0)
        grad_weights = dot(values, grads, 1, 1)
        delta = jnp.sum(weights * grad_weights, axis=0, keepdims=True)
        grad_scores = (weights * (grad_weights - delta)).astype(jnp.bfloat16)
        grad_query = dot(keys, grad_scores, 0, 0) * scaling
        grad_key = dot(grad_scores, queries, 1, 0) * scaling
        grad_value = dot(weights_bf, grads, 1, 0)
        for k in range(1, back + 1):
            at = slice((back - k) * rows, (back - k + 1) * rows)
            part[k - 1, g, 0] = grad_key[at].astype(jnp.bfloat16)
            part[k - 1, g, 1] = grad_value[at].astype(jnp.bfloat16)
        own[g, 0] = grad_key[back * rows :]
        own[g, 1] = grad_value[back * rows :]

        @pl.when(g % per == per - 1)
        def _():
            for k in range(1, back + 1):
                @pl.when(me - k >= 0)
                def _():
                    g_copy(g // per, k).start()

        for h in range(groups):
            at = slice(h * HEAD_DIM, (h + 1) * HEAD_DIM)
            to = columns(g * groups + h, HEAD_DIM)
            attbuf[:, to] = attended[:, at].T.astype(jnp.bfloat16)
            dqbuf[:, to] = grad_query[:, at].T.astype(jnp.bfloat16)

    @pl.loop(0, chunks)
    def _(c):
        for k in range(1, back + 1):
            @pl.when(me + k < total)
            def _():
                g_copy(c, k).wait_recv()
        for i in range(per):
            g = c * per + i
            sums = own[g]
            for k in range(1, back + 1):
                sums = sums + landed[k - 1, g].astype(jnp.float32)
            dkbuf[:, columns(g, HEAD_DIM)] = sums[0].astype(jnp.bfloat16)
            dvbuf[:, columns(g, HEAD_DIM)] = sums[1].astype(jnp.bfloat16)

    @pl.when(relays)
    def _():
        relay().wait_send()

    @pl.loop(0, chunks)
    def _(c):
        for k in range(1, back + 1):
            direct = jnp.logical_not(edge & (c == last)) if k == 1 else True
            @pl.when((me + k < total) & direct)
            def _():
                kv_copy(c, k).wait_send()

            @pl.when(me - k >= 0)
            def _():
                g_copy(c, k).wait_send()


def write_out(att, dq, dk, dv, att_hbm, dq_hbm, dk_hbm, dv_hbm, sems):
    pairs = ((att, att_hbm), (dq, dq_hbm), (dk, dk_hbm), (dv, dv_hbm))
    copies = [
        pltpu.make_async_copy(source, target, sems.at[which])
        for which, (source, target) in enumerate(pairs)
    ]
    for copy in copies:
        copy.start()
    for copy in copies:
        copy.wait()


def solution(mesh):
    back = mesh.shape["head"]
    total = mesh.shape["blk"] * back

    def per_device(query, key, value, grad_out, doc_lengths):
        rows, kv_heads = query.shape[0], key.shape[1] // HEAD_DIM
        width = query.shape[1] // kv_heads
        chunks = kv_heads // math.gcd(kv_heads, HEADS_A_COPY)
        bf, f32 = jnp.bfloat16, jnp.float32
        anywhere = pl.BlockSpec(memory_space=pl.ANY)
        dma = pltpu.SemaphoreType.DMA
        results = pl.pallas_call(
            functools.partial(kernel, back, total),
            out_shape=[
                pltpu.VMEM(query.shape, bf),
                pltpu.VMEM(query.shape, bf),
                pltpu.VMEM(key.shape, bf),
                pltpu.VMEM(key.shape, bf),
            ],
            in_specs=[anywhere] * 5,
            out_specs=[pl.BlockSpec(memory_space=pltpu.VMEM)] * 4,
            scratch_shapes=[
                pltpu.VMEM((back + 1, kv_heads, 2, rows, HEAD_DIM), bf),
                pltpu.VMEM((kv_heads, rows, width), bf),
                pltpu.VMEM((kv_heads, rows, width), bf),
                pltpu.VMEM((back, kv_heads, 2, rows, HEAD_DIM), bf),
                pltpu.VMEM((back, kv_heads, 2, rows, HEAD_DIM), bf),
                pltpu.VMEM((kv_heads, 2, rows, HEAD_DIM), f32),
                pltpu.VMEM(((back + 1) * rows, rows), f32),
                pltpu.SMEM(doc_lengths.shape, jnp.int32),
                dma,
                dma((2, kv_heads)),
                dma((2, kv_heads)),
                dma((back, chunks)),
                dma((back, chunks)),
                dma,
                dma((back, chunks)),
                dma((back, chunks)),
            ],
            compiler_params=pltpu.CompilerParams(collective_id=0, has_side_effects=True),
        )(doc_lengths, query, key, value, grad_out)
        results = [pltpu.with_memory_space_constraint(r, pltpu.VMEM) for r in results]
        return pl.pallas_call(
            write_out,
            out_shape=[
                jax.ShapeDtypeStruct(query.shape, bf),
                jax.ShapeDtypeStruct(query.shape, bf),
                jax.ShapeDtypeStruct(key.shape, bf),
                jax.ShapeDtypeStruct(key.shape, bf),
            ],
            in_specs=[pl.BlockSpec(memory_space=pltpu.VMEM)] * 4,
            out_specs=[anywhere] * 4,
            scratch_shapes=[dma((4,))],
        )(*results)

    split = P(("blk", "head"), None)
    return jax.shard_map(
        per_device,
        mesh=mesh,
        in_specs=(split, split, split, split, P()),
        out_specs=(split, split, split, split),
        check_vma=False,
    )
```

```python
import functools
import math

import jax
import jax.numpy as jnp
from jax import lax
from jax.experimental import pallas as pl
from jax.experimental.pallas import tpu as pltpu
from jax.sharding import PartitionSpec as P

HEAD_DIM = 128
EXCLUDED = -1e30
HEADS_A_COPY = 2
MESH = pl.DeviceIdType.MESH


def kernel(
    back, total, lens_hbm, q_hbm, k_hbm, v_hbm, do_hbm, attbuf, dqbuf, dkbuf, dvbuf,
    window, qbuf, dobuf, part, landed, own, bias, lens,
    lens_in, kv_in, q_in, kv_send, kv_recv, relay_send, g_send, g_recv,
):
    rows = q_hbm.shape[0]
    kv_heads = k_hbm.shape[1] // HEAD_DIM
    groups = q_hbm.shape[1] // k_hbm.shape[1]
    span = (back + 1) * rows
    scaling = HEAD_DIM ** (-0.5)
    chunks = kv_recv.shape[1]
    per = kv_heads // chunks
    last = chunks - 1
    me = lax.axis_index("blk") * back + lax.axis_index("head")
    place = me % (2 * back)
    edge = (place == 2 * back - 1) & (me + back < total) & (back == 2)
    relays = (place == 1) & (me > back) & (back == 2)

    def device(number):
        return {"blk": number // back, "head": number % back}

    def columns(g, size):
        return pl.ds(pl.multiple_of(g * size, size), size)

    def heads(c):
        return pl.ds(c * per, per)

    def kv_load(g, which):
        return pltpu.make_async_copy(
            (k_hbm, v_hbm)[which].at[:, columns(g, HEAD_DIM)],
            window.at[0, g, which],
            kv_in.at[jnp.minimum(g // per, 1)],
        )

    q_load = pltpu.make_async_copy(q_hbm, qbuf, q_in.at[0])
    do_load = pltpu.make_async_copy(do_hbm, dobuf, q_in.at[1])

    def loaded(at, which):
        pltpu.make_async_copy(window.at[0, at], window.at[0, at], kv_in.at[which]).wait()

    def kv_copy(c, k):
        return pltpu.make_async_remote_copy(
            src_ref=window.at[0, heads(c)],
            dst_ref=window.at[k, heads(c)],
            send_sem=kv_send.at[k - 1],
            recv_sem=kv_recv.at[k - 1, c],
            device_id=device(me + k),
            device_id_type=MESH,
        )

    def relay():
        return pltpu.make_async_remote_copy(
            src_ref=window.at[back, heads(last)],
            dst_ref=window.at[1, heads(last)],
            send_sem=relay_send,
            recv_sem=kv_recv.at[0, last],
            device_id=device(me - 1),
            device_id_type=MESH,
        )

    def g_copy(c, k):
        return pltpu.make_async_remote_copy(
            src_ref=part.at[k - 1, heads(c)],
            dst_ref=landed.at[k - 1, heads(c)],
            send_sem=g_send.at[k - 1],
            recv_sem=g_recv.at[k - 1, c],
            device_id=device(me - k),
            device_id_type=MESH,
        )

    barrier = pltpu.get_barrier_semaphore()
    for k in range(1, back + 1):
        @pl.when(me - k >= 0)
        def _():
            pl.semaphore_signal(barrier, inc=1, device_id=device(me - k), device_id_type=MESH)

    @pl.loop(0, kv_heads)
    def _(g):
        kv_load(g, 0).start()
        kv_load(g, 1).start()

    lens_load = pltpu.make_async_copy(lens_hbm, lens, lens_in)
    lens_load.start()

    q_load.start()
    do_load.start()

    @pl.when(me < total - 1)
    def _():
        pl.semaphore_wait(barrier, jnp.minimum(total - 1 - me, back))

    def send(c):
        for k in range(1, back + 1):
            @pl.when(me + k < total)
            def _():
                kv_copy(c, k).start()

    loaded(heads(0), 0)

    @pl.when(jnp.logical_not(edge))
    def _():
        send(0)

    loaded(pl.ds(per, kv_heads - per), 1)

    @pl.when(edge)
    def _():
        kv_copy(last, back).start()
        send(0)

    @pl.loop(1, chunks - edge.astype(jnp.int32))
    def _(c):
        send(c)

    for k in range(1, back + 1):
        @pl.when(me - k < 0)
        def _():
            window[k] = jnp.zeros((kv_heads, 2, rows, HEAD_DIM), jnp.bfloat16)

        @pl.when(me + k >= total)
        def _():
            landed[k - 1] = jnp.zeros((kv_heads, 2, rows, HEAD_DIM), jnp.bfloat16)

    lens_load.wait()
    query_pos = me * rows + lax.broadcasted_iota(jnp.int32, (1, rows), 1)

    def latest(d, carry):
        start, first = carry
        return start + lens[d], jnp.where(query_pos >= start, start, first)

    _, first = lax.fori_loop(
        0, lens.shape[0], latest, (jnp.int32(0), jnp.zeros((1, rows), jnp.int32))
    )
    key_pos = (me - back) * rows + lax.broadcasted_iota(jnp.int32, (span, rows), 0)
    bias[...] = jnp.where((key_pos <= query_pos) & (key_pos >= first), 0.0, EXCLUDED)

    def dot(a, b, a_dim, b_dim):
        return lax.dot_general(
            a, b, (((a_dim,), (b_dim,)), ((), ())), preferred_element_type=jnp.float32
        )

    def stacked(buf, g):
        return jnp.concatenate(
            [buf[:, columns(g * groups + h, HEAD_DIM)] for h in range(groups)], axis=0
        )

    q_load.wait()
    do_load.wait()

    @pl.loop(0, kv_heads)
    def _(g):
        @pl.when(g % per == 0)
        def _():
            for k in range(1, back + 1):
                early = relays & (g // per == last) if k == back else False
                @pl.when((me - k >= 0) & jnp.logical_not(early))
                def _():
                    kv_copy(g // per, k).wait_recv()

        @pl.when(relays & (g == 0))
        def _():
            kv_copy(last, back).wait_recv()
            relay().start()

        keys, values = (
            jnp.concatenate([window[k, g, which] for k in range(back, -1, -1)], axis=0)
            for which in range(2)
        )
        queries, grads = stacked(qbuf, g), stacked(dobuf, g)
        kept = jnp.concatenate([bias[...]] * groups, axis=1)
        scores = dot(keys, queries, 1, 1) * (scaling * math.log2(math.e)) + kept
        peak = jnp.max(scores, axis=0, keepdims=True)
        raised = jnp.exp2(scores - peak)
        weights = raised * (1.0 / jnp.sum(raised, axis=0, keepdims=True))
        weights_bf = weights.astype(jnp.bfloat16)
        attended = dot(values, weights_bf, 0, 0)
        grad_weights = dot(values, grads, 1, 1)
        delta = jnp.sum(weights * grad_weights, axis=0, keepdims=True)
        grad_scores = (weights * (grad_weights - delta)).astype(jnp.bfloat16)
        grad_query = dot(keys, grad_scores, 0, 0) * scaling
        grad_key = dot(grad_scores, queries, 1, 0) * scaling
        grad_value = dot(weights_bf, grads, 1, 0)
        for k in range(1, back + 1):
            at = slice((back - k) * rows, (back - k + 1) * rows)
            part[k - 1, g, 0] = grad_key[at].astype(jnp.bfloat16)
            part[k - 1, g, 1] = grad_value[at].astype(jnp.bfloat16)
        own[g, 0] = grad_key[back * rows :]
        own[g, 1] = grad_value[back * rows :]

        @pl.when(g % per == per - 1)
        def _():
            for k in range(1, back + 1):
                @pl.when(me - k >= 0)
                def _():
                    g_copy(g // per, k).start()

        for h in range(groups):
            at = slice(h * HEAD_DIM, (h + 1) * HEAD_DIM)
            to = columns(g * groups + h, HEAD_DIM)
            attbuf[:, to] = attended[:, at].T.astype(jnp.bfloat16)
            dqbuf[:, to] = grad_query[:, at].T.astype(jnp.bfloat16)

    @pl.loop(0, chunks)
    def _(c):
        for k in range(1, back + 1):
            @pl.when(me + k < total)
            def _():
                g_copy(c, k).wait_recv()
        for i in range(per):
            g = c * per + i
            sums = own[g]
            for k in range(1, back + 1):
                sums = sums + landed[k - 1, g].astype(jnp.float32)
            dkbuf[:, columns(g, HEAD_DIM)] = sums[0].astype(jnp.bfloat16)
            dvbuf[:, columns(g, HEAD_DIM)] = sums[1].astype(jnp.bfloat16)

    @pl.when(relays)
    def _():
        relay().wait_send()

    for k in range(1, back + 1):
        def sent(count):
            pltpu.make_async_copy(
                window.at[0, pl.ds(0, count)], window.at[0, pl.ds(0, count)], kv_send.at[k - 1]
            ).wait()

        short = edge if k == 1 else jnp.bool_(False)

        @pl.when((me + k < total) & jnp.logical_not(short))
        def _():
            sent(kv_heads)

        @pl.when(short)
        def _():
            sent(last * per)

        @pl.when(me - k >= 0)
        def _():
            pltpu.make_async_copy(part.at[k - 1], part.at[k - 1], g_send.at[k - 1]).wait()


def write_out(att, dq, dk, dv, att_hbm, dq_hbm, dk_hbm, dv_hbm, sems):
    pairs = ((att, att_hbm), (dq, dq_hbm), (dk, dk_hbm), (dv, dv_hbm))
    copies = [
        pltpu.make_async_copy(source, target, sems.at[which])
        for which, (source, target) in enumerate(pairs)
    ]
    for copy in copies:
        copy.start()
    for copy in copies:
        copy.wait()


def solution(mesh):
    back = mesh.shape["head"]
    total = mesh.shape["blk"] * back

    def per_device(query, key, value, grad_out, doc_lengths):
        rows, kv_heads = query.shape[0], key.shape[1] // HEAD_DIM
        chunks = kv_heads // math.gcd(kv_heads, HEADS_A_COPY)
        bf, f32 = jnp.bfloat16, jnp.float32
        anywhere = pl.BlockSpec(memory_space=pl.ANY)
        dma = pltpu.SemaphoreType.DMA
        results = pl.pallas_call(
            functools.partial(kernel, back, total),
            out_shape=[
                pltpu.VMEM(query.shape, bf),
                pltpu.VMEM(query.shape, bf),
                pltpu.VMEM(key.shape, bf),
                pltpu.VMEM(key.shape, bf),
            ],
            in_specs=[anywhere] * 5,
            out_specs=[pl.BlockSpec(memory_space=pltpu.VMEM)] * 4,
            scratch_shapes=[
                pltpu.VMEM((back + 1, kv_heads, 2, rows, HEAD_DIM), bf),
                pltpu.VMEM(query.shape, bf),
                pltpu.VMEM(query.shape, bf),
                pltpu.VMEM((back, kv_heads, 2, rows, HEAD_DIM), bf),
                pltpu.VMEM((back, kv_heads, 2, rows, HEAD_DIM), bf),
                pltpu.VMEM((kv_heads, 2, rows, HEAD_DIM), f32),
                pltpu.VMEM(((back + 1) * rows, rows), f32),
                pltpu.SMEM(doc_lengths.shape, jnp.int32),
                dma,
                dma((2,)),
                dma((2,)),
                dma((back,)),
                dma((back, chunks)),
                dma,
                dma((back,)),
                dma((back, chunks)),
            ],
            compiler_params=pltpu.CompilerParams(collective_id=0, has_side_effects=True),
        )(doc_lengths, query, key, value, grad_out)
        results = [pltpu.with_memory_space_constraint(r, pltpu.VMEM) for r in results]
        return pl.pallas_call(
            write_out,
            out_shape=[
                jax.ShapeDtypeStruct(query.shape, bf),
                jax.ShapeDtypeStruct(query.shape, bf),
                jax.ShapeDtypeStruct(key.shape, bf),
                jax.ShapeDtypeStruct(key.shape, bf),
            ],
            in_specs=[pl.BlockSpec(memory_space=pltpu.VMEM)] * 4,
            out_specs=[anywhere] * 4,
            scratch_shapes=[dma((4,))],
        )(*results)

    split = P(("blk", "head"), None)
    return jax.shard_map(
        per_device,
        mesh=mesh,
        in_specs=(split, split, split, split, P()),
        out_specs=(split, split, split, split),
        check_vma=False,
    )
```

```python
import functools
import math

import jax
import jax.numpy as jnp
from jax import lax
from jax.experimental import pallas as pl
from jax.experimental.pallas import tpu as pltpu
from jax.sharding import PartitionSpec as P

HEAD_DIM = 128
EXCLUDED = -1e30
HEADS_A_COPY = 2
MESH = pl.DeviceIdType.MESH


def kernel(
    back, total, lens_hbm, q_hbm, k_hbm, v_hbm, do_hbm, attbuf, dqbuf, dkbuf, dvbuf,
    window, qbuf, dobuf, part, landed, passing, own, bias, lens,
    lens_in, kv_in, q_in, kv_send, kv_recv, relay_send, g_send, g_recv, pass_recv, pass_send,
):
    rows = q_hbm.shape[0]
    kv_heads = k_hbm.shape[1] // HEAD_DIM
    groups = q_hbm.shape[1] // k_hbm.shape[1]
    span = (back + 1) * rows
    scaling = HEAD_DIM ** (-0.5)
    chunks = kv_recv.shape[1]
    per = kv_heads // chunks
    last = chunks - 1
    me = lax.axis_index("blk") * back + lax.axis_index("head")
    place = me % (2 * back)
    edge = (place == 2 * back - 1) & (me + back < total) & (back == 2)
    relays = (place == 1) & (me > back) & (back == 2)
    around = (place == 0) & (me > back) & (back == 2)
    passes = (place == 2) & (me + back < total) & (back == 2)

    def device(number):
        return {"blk": number // back, "head": number % back}

    def columns(g, size):
        return pl.ds(pl.multiple_of(g * size, size), size)

    def heads(c):
        return pl.ds(c * per, per)

    def kv_load(g, which):
        return pltpu.make_async_copy(
            (k_hbm, v_hbm)[which].at[:, columns(g, HEAD_DIM)],
            window.at[0, g, which],
            kv_in.at[jnp.minimum(g // per, 1)],
        )

    q_load = pltpu.make_async_copy(q_hbm, qbuf, q_in.at[0])
    do_load = pltpu.make_async_copy(do_hbm, dobuf, q_in.at[1])

    def loaded(at, which):
        pltpu.make_async_copy(window.at[0, at], window.at[0, at], kv_in.at[which]).wait()

    def kv_copy(c, k):
        return pltpu.make_async_remote_copy(
            src_ref=window.at[0, heads(c)],
            dst_ref=window.at[k, heads(c)],
            send_sem=kv_send.at[k - 1],
            recv_sem=kv_recv.at[k - 1, c],
            device_id=device(me + k),
            device_id_type=MESH,
        )

    def first_copy(g, which, k):
        return pltpu.make_async_remote_copy(
            src_ref=(k_hbm, v_hbm)[which].at[:, columns(g, HEAD_DIM)],
            dst_ref=window.at[k, g, which],
            send_sem=kv_send.at[k - 1],
            recv_sem=kv_recv.at[k - 1, 0],
            device_id=device(me + k),
            device_id_type=MESH,
        )

    def relay():
        return pltpu.make_async_remote_copy(
            src_ref=window.at[back, heads(last)],
            dst_ref=window.at[1, heads(last)],
            send_sem=relay_send,
            recv_sem=kv_recv.at[0, last],
            device_id=device(me - 1),
            device_id_type=MESH,
        )

    def g_copy(g, k):
        return pltpu.make_async_remote_copy(
            src_ref=part.at[k - 1, g],
            dst_ref=landed.at[k - 1, g],
            send_sem=g_send.at[k - 1],
            recv_sem=g_recv.at[k - 1, g // per],
            device_id=device(me - k),
            device_id_type=MESH,
        )

    def g_landed(c, k):
        at = landed.at[k - 1, heads(c)]
        pltpu.make_async_copy(at, at, g_recv.at[k - 1, c]).wait()

    barrier = pltpu.get_barrier_semaphore()
    for k in range(1, back + 1):
        @pl.when(me - k >= 0)
        def _():
            pl.semaphore_signal(barrier, inc=1, device_id=device(me - k), device_id_type=MESH)

    around_copy = pltpu.make_async_remote_copy(
        src_ref=part.at[0, heads(0)],
        dst_ref=passing,
        send_sem=g_send.at[0],
        recv_sem=pass_recv,
        device_id=device(me - back),
        device_id_type=MESH,
    )
    pass_copy = pltpu.make_async_remote_copy(
        src_ref=passing,
        dst_ref=landed.at[0, heads(0)],
        send_sem=pass_send,
        recv_sem=g_recv.at[0, 0],
        device_id=device(me + 1),
        device_id_type=MESH,
    )

    @pl.loop(0, kv_heads)
    def _(g):
        kv_load(g, 0).start()
        kv_load(g, 1).start()

    lens_load = pltpu.make_async_copy(lens_hbm, lens, lens_in)
    lens_load.start()


    @pl.when(me < total - 1)
    def _():
        pl.semaphore_wait(barrier, jnp.minimum(total - 1 - me, back))

    def first(k):
        for g in range(per):
            for which in range(2):
                first_copy(g, which, k).start()

    for k in range(1, back + 1):
        @pl.when((me + k < total) & jnp.logical_not(edge if k == back else False))
        def _():
            first(k)

    q_load.start()
    do_load.start()
    loaded(heads(0), 0)
    loaded(pl.ds(per, kv_heads - per), 1)

    @pl.when(edge)
    def _():
        kv_copy(last, back).start()
        first(back)

    @pl.loop(1, chunks - edge.astype(jnp.int32))
    def _(c):
        for k in range(1, back + 1):
            later = relays & (c == last) if k == 1 else False
            @pl.when((me + k < total) & jnp.logical_not(later))
            def _():
                kv_copy(c, k).start()

    for k in range(1, back + 1):
        @pl.when(me - k < 0)
        def _():
            window[k] = jnp.zeros((kv_heads, 2, rows, HEAD_DIM), jnp.bfloat16)

        @pl.when(me + k >= total)
        def _():
            landed[k - 1] = jnp.zeros((kv_heads, 2, rows, HEAD_DIM), jnp.bfloat16)

    lens_load.wait()
    query_pos = me * rows + lax.broadcasted_iota(jnp.int32, (1, rows), 1)

    def latest(d, carry):
        start, first = carry
        return start + lens[d], jnp.where(query_pos >= start, start, first)

    _, first = lax.fori_loop(
        0, lens.shape[0], latest, (jnp.int32(0), jnp.zeros((1, rows), jnp.int32))
    )
    key_pos = (me - back) * rows + lax.broadcasted_iota(jnp.int32, (span, rows), 0)
    bias[...] = jnp.where((key_pos <= query_pos) & (key_pos >= first), 0.0, EXCLUDED)

    def dot(a, b, a_dim, b_dim):
        return lax.dot_general(
            a, b, (((a_dim,), (b_dim,)), ((), ())), preferred_element_type=jnp.float32
        )

    def stacked(buf, g):
        return jnp.concatenate(
            [buf[:, columns(g * groups + h, HEAD_DIM)] for h in range(groups)], axis=0
        )

    q_load.wait()
    do_load.wait()

    @pl.loop(0, kv_heads)
    def _(g):
        @pl.when(g % per == 0)
        def _():
            for k in range(1, back + 1):
                early = relays & (g // per == last) if k == back else False
                @pl.when((me - k >= 0) & jnp.logical_not(early))
                def _():
                    kv_copy(g // per, k).wait_recv()

        @pl.when(relays & (g == 0))
        def _():
            kv_copy(last, back).wait_recv()
            relay().start()
            kv_copy(last, 1).start()

        @pl.when(passes & (g == kv_heads - 1))
        def _():
            around_copy.wait_recv()
            pass_copy.start()

        keys, values = (
            jnp.concatenate([window[k, g, which] for k in range(back, -1, -1)], axis=0)
            for which in range(2)
        )
        queries, grads = stacked(qbuf, g), stacked(dobuf, g)
        kept = jnp.concatenate([bias[...]] * groups, axis=1)
        scores = dot(keys, queries, 1, 1) * (scaling * math.log2(math.e)) + kept
        peak = jnp.max(scores, axis=0, keepdims=True)
        raised = jnp.exp2(scores - peak)
        weights = raised * (1.0 / jnp.sum(raised, axis=0, keepdims=True))
        weights_bf = weights.astype(jnp.bfloat16)
        attended = dot(values, weights_bf, 0, 0)
        grad_weights = dot(values, grads, 1, 1)
        delta = jnp.sum(weights * grad_weights, axis=0, keepdims=True)
        grad_scores = (weights * (grad_weights - delta)).astype(jnp.bfloat16)
        grad_query = dot(keys, grad_scores, 0, 0) * scaling
        grad_key = dot(grad_scores, queries, 1, 0) * scaling
        grad_value = dot(weights_bf, grads, 1, 0)
        for k in range(1, back + 1):
            at = slice((back - k) * rows, (back - k + 1) * rows)
            part[k - 1, g, 0] = grad_key[at].astype(jnp.bfloat16)
            part[k - 1, g, 1] = grad_value[at].astype(jnp.bfloat16)
        own[g, 0] = grad_key[back * rows :]
        own[g, 1] = grad_value[back * rows :]

        @pl.when(around & (g == per - 1))
        def _():
            around_copy.start()

        for k in range(back, 0, -1):
            detour = around & (g < per) if k == 1 else False
            @pl.when((me - k >= 0) & jnp.logical_not(detour))
            def _():
                g_copy(g, k).start()

        for h in range(groups):
            at = slice(h * HEAD_DIM, (h + 1) * HEAD_DIM)
            to = columns(g * groups + h, HEAD_DIM)
            attbuf[:, to] = attended[:, at].T.astype(jnp.bfloat16)
            dqbuf[:, to] = grad_query[:, at].T.astype(jnp.bfloat16)

    @pl.loop(0, chunks)
    def _(c):
        for k in range(1, back + 1):
            @pl.when(me + k < total)
            def _():
                g_landed(c, k)
        for i in range(per):
            g = c * per + i
            sums = own[g]
            for k in range(1, back + 1):
                sums = sums + landed[k - 1, g].astype(jnp.float32)
            dkbuf[:, columns(g, HEAD_DIM)] = sums[0].astype(jnp.bfloat16)
            dvbuf[:, columns(g, HEAD_DIM)] = sums[1].astype(jnp.bfloat16)

    @pl.when(relays)
    def _():
        relay().wait_send()

    @pl.when(passes)
    def _():
        pass_copy.wait_send()

    for k in range(1, back + 1):
        def sent(count):
            pltpu.make_async_copy(
                window.at[0, pl.ds(0, count)], window.at[0, pl.ds(0, count)], kv_send.at[k - 1]
            ).wait()

        short = edge if k == 1 else jnp.bool_(False)

        @pl.when((me + k < total) & jnp.logical_not(short))
        def _():
            sent(kv_heads)

        @pl.when(short)
        def _():
            sent(last * per)

        @pl.when(me - k >= 0)
        def _():
            pltpu.make_async_copy(part.at[k - 1], part.at[k - 1], g_send.at[k - 1]).wait()


def write_out(att, dq, dk, dv, att_hbm, dq_hbm, dk_hbm, dv_hbm, sems):
    pairs = ((att, att_hbm), (dq, dq_hbm), (dk, dk_hbm), (dv, dv_hbm))
    copies = [
        pltpu.make_async_copy(source, target, sems.at[which])
        for which, (source, target) in enumerate(pairs)
    ]
    for copy in copies:
        copy.start()
    for copy in copies:
        copy.wait()


def solution(mesh):
    back = mesh.shape["head"]
    total = mesh.shape["blk"] * back

    def per_device(query, key, value, grad_out, doc_lengths):
        rows, kv_heads = query.shape[0], key.shape[1] // HEAD_DIM
        chunks = kv_heads // math.gcd(kv_heads, HEADS_A_COPY)
        bf, f32 = jnp.bfloat16, jnp.float32
        anywhere = pl.BlockSpec(memory_space=pl.ANY)
        dma = pltpu.SemaphoreType.DMA
        results = pl.pallas_call(
            functools.partial(kernel, back, total),
            out_shape=[
                pltpu.VMEM(query.shape, bf),
                pltpu.VMEM(query.shape, bf),
                pltpu.VMEM(key.shape, bf),
                pltpu.VMEM(key.shape, bf),
            ],
            in_specs=[anywhere] * 5,
            out_specs=[pl.BlockSpec(memory_space=pltpu.VMEM)] * 4,
            scratch_shapes=[
                pltpu.VMEM((back + 1, kv_heads, 2, rows, HEAD_DIM), bf),
                pltpu.VMEM(query.shape, bf),
                pltpu.VMEM(query.shape, bf),
                pltpu.VMEM((back, kv_heads, 2, rows, HEAD_DIM), bf),
                pltpu.VMEM((back, kv_heads, 2, rows, HEAD_DIM), bf),
                pltpu.VMEM((kv_heads // chunks, 2, rows, HEAD_DIM), bf),
                pltpu.VMEM((kv_heads, 2, rows, HEAD_DIM), f32),
                pltpu.VMEM(((back + 1) * rows, rows), f32),
                pltpu.SMEM(doc_lengths.shape, jnp.int32),
                dma,
                dma((2,)),
                dma((2,)),
                dma((back,)),
                dma((back, chunks)),
                dma,
                dma((back,)),
                dma((back, chunks)),
                dma,
                dma,
            ],
            compiler_params=pltpu.CompilerParams(collective_id=0, has_side_effects=True),
        )(doc_lengths, query, key, value, grad_out)
        results = [pltpu.with_memory_space_constraint(r, pltpu.VMEM) for r in results]
        return pl.pallas_call(
            write_out,
            out_shape=[
                jax.ShapeDtypeStruct(query.shape, bf),
                jax.ShapeDtypeStruct(query.shape, bf),
                jax.ShapeDtypeStruct(key.shape, bf),
                jax.ShapeDtypeStruct(key.shape, bf),
            ],
            in_specs=[pl.BlockSpec(memory_space=pltpu.VMEM)] * 4,
            out_specs=[anywhere] * 4,
            scratch_shapes=[dma((4,))],
        )(*results)

    split = P(("blk", "head"), None)
    return jax.shard_map(
        per_device,
        mesh=mesh,
        in_specs=(split, split, split, split, P()),
        out_specs=(split, split, split, split),
        check_vma=False,
    )
```

```python
import functools
import math

import jax
import jax.numpy as jnp
from jax import lax
from jax.experimental import pallas as pl
from jax.experimental.pallas import tpu as pltpu
from jax.sharding import PartitionSpec as P

HEAD_DIM = 128
EXCLUDED = -1e30
HEADS_A_COPY = 2
MESH = pl.DeviceIdType.MESH


def kernel(
    back, total, lens_hbm, q_hbm, k_hbm, v_hbm, do_hbm, attbuf, dqbuf, dkbuf, dvbuf,
    window, qbuf, part, landed, passing, own, bias, lens,
    lens_in, kv_in, q_in, kv_send, kv_recv, edge_recv, relay_send, g_send, g_recv, pass_recv, pass_send,
):
    rows = q_hbm.shape[0]
    kv_heads = k_hbm.shape[1] // HEAD_DIM
    groups = q_hbm.shape[1] // k_hbm.shape[1]
    span = (back + 1) * rows
    scaling = HEAD_DIM ** (-0.5)
    chunks = g_recv.shape[0]
    per = kv_heads // chunks
    last = chunks - 1
    me = lax.axis_index("blk") * back + lax.axis_index("head")
    place = me % (2 * back)
    edge = (place == 2 * back - 1) & (me + back < total) & (back == 2)
    relays = (place == 1) & (me > back) & (back == 2)
    around = (place == 0) & (me > back) & (back == 2)
    passes = (place == 2) & (me + back < total) & (back == 2)

    def device(number):
        return {"blk": number // back, "head": number % back}

    def columns(g, size):
        return pl.ds(pl.multiple_of(g * size, size), size)

    def heads(c):
        return pl.ds(c * per, per)

    def kv_load(g, which):
        return pltpu.make_async_copy(
            (k_hbm, v_hbm)[which].at[:, columns(g, HEAD_DIM)],
            window.at[0, g, which],
            kv_in,
        )

    q_load = pltpu.make_async_copy(q_hbm, qbuf.at[0], q_in)
    do_load = pltpu.make_async_copy(do_hbm, qbuf.at[1], q_in)

    def wait_for(landing, sem):
        pltpu.make_async_copy(landing, landing, sem).wait()

    def kv_copy(c, k):
        return pltpu.make_async_remote_copy(
            src_ref=window.at[0, heads(c)],
            dst_ref=window.at[k, heads(c)],
            send_sem=kv_send.at[k - 1],
            recv_sem=kv_recv.at[c],
            device_id=device(me + k),
            device_id_type=MESH,
        )

    def first_copy(g, which, k):
        return pltpu.make_async_remote_copy(
            src_ref=(k_hbm, v_hbm)[which].at[:, columns(g, HEAD_DIM)],
            dst_ref=window.at[k, g, which],
            send_sem=kv_send.at[k - 1],
            recv_sem=kv_recv.at[0],
            device_id=device(me + k),
            device_id_type=MESH,
        )

    edge_copy = pltpu.make_async_remote_copy(
        src_ref=window.at[0, heads(last)],
        dst_ref=window.at[back, heads(last)],
        send_sem=kv_send.at[back - 1],
        recv_sem=edge_recv,
        device_id=device(me + back),
        device_id_type=MESH,
    )

    def relay():
        return pltpu.make_async_remote_copy(
            src_ref=window.at[back, heads(last)],
            dst_ref=window.at[1, heads(last)],
            send_sem=relay_send,
            recv_sem=kv_recv.at[last],
            device_id=device(me - 1),
            device_id_type=MESH,
        )

    def g_copy(g, k):
        return pltpu.make_async_remote_copy(
            src_ref=part.at[k - 1, g],
            dst_ref=landed.at[k - 1, g],
            send_sem=g_send.at[k - 1],
            recv_sem=g_recv.at[g // per],
            device_id=device(me - k),
            device_id_type=MESH,
        )

    barrier = pltpu.get_barrier_semaphore()
    for k in range(1, back + 1):
        @pl.when(me - k >= 0)
        def _():
            pl.semaphore_signal(barrier, inc=1, device_id=device(me - k), device_id_type=MESH)

    around_copy = pltpu.make_async_remote_copy(
        src_ref=part.at[0, heads(0)],
        dst_ref=passing,
        send_sem=g_send.at[0],
        recv_sem=pass_recv,
        device_id=device(me - back),
        device_id_type=MESH,
    )
    pass_copy = pltpu.make_async_remote_copy(
        src_ref=passing,
        dst_ref=landed.at[0, heads(0)],
        send_sem=pass_send,
        recv_sem=g_recv.at[0],
        device_id=device(me + 1),
        device_id_type=MESH,
    )

    @pl.when(place != 1)
    def _():
        @pl.loop(0, kv_heads)
        def _(g):
            kv_load(g, 0).start()
            kv_load(g, 1).start()

    lens_load = pltpu.make_async_copy(lens_hbm, lens, lens_in)
    lens_load.start()


    @pl.when(me < total - 1)
    def _():
        pl.semaphore_wait(barrier, jnp.minimum(total - 1 - me, back))

    def first(k):
        for g in range(per):
            for which in range(2):
                first_copy(g, which, k).start()

    for k in range(1, back + 1):
        @pl.when((me + k < total) & jnp.logical_not(edge if k == back else False))
        def _():
            first(k)

    @pl.when(place == 1)
    def _():
        @pl.loop(0, kv_heads)
        def _(g):
            kv_load(g, 0).start()
            kv_load(g, 1).start()

    wait_for(window.at[0], kv_in)

    @pl.when(edge)
    def _():
        edge_copy.start()
        first(back)

    @pl.loop(1, chunks - edge.astype(jnp.int32))
    def _(c):
        for k in range(1, back + 1):
            later = relays & (c == last) if k == 1 else False
            @pl.when((me + k < total) & jnp.logical_not(later))
            def _():
                kv_copy(c, k).start()

    q_load.start()
    do_load.start()

    for k in range(1, back + 1):
        @pl.when(me - k < 0)
        def _():
            window[k] = jnp.zeros((kv_heads, 2, rows, HEAD_DIM), jnp.bfloat16)

        @pl.when(me + k >= total)
        def _():
            landed[k - 1] = jnp.zeros((kv_heads, 2, rows, HEAD_DIM), jnp.bfloat16)

    lens_load.wait()
    query_pos = me * rows + lax.broadcasted_iota(jnp.int32, (1, rows), 1)

    def latest(d, carry):
        start, first = carry
        return start + lens[d], jnp.where(query_pos >= start, start, first)

    _, first = lax.fori_loop(
        0, lens.shape[0], latest, (jnp.int32(0), jnp.zeros((1, rows), jnp.int32))
    )
    key_pos = (me - back) * rows + lax.broadcasted_iota(jnp.int32, (span, rows), 0)
    bias[...] = jnp.where((key_pos <= query_pos) & (key_pos >= first), 0.0, EXCLUDED)

    def dot(a, b, a_dim, b_dim):
        return lax.dot_general(
            a, b, (((a_dim,), (b_dim,)), ((), ())), preferred_element_type=jnp.float32
        )

    def stacked(which, g):
        return jnp.concatenate(
            [qbuf[which, :, columns(g * groups + h, HEAD_DIM)] for h in range(groups)], axis=0
        )

    wait_for(qbuf, q_in)

    @pl.loop(0, kv_heads)
    def _(g):
        @pl.when(g % per == 0)
        def _():
            early = relays & (g == last * per)
            for n in range(1, back + 1):
                @pl.when((jnp.minimum(me, back) - early.astype(jnp.int32)) == n)
                def _():
                    wait_for(window.at[pl.ds(1, n), heads(g // per)], kv_recv.at[g // per])

        @pl.when(relays & (g == 0))
        def _():
            edge_copy.wait_recv()
            relay().start()
            kv_copy(last, 1).start()

        @pl.when(passes & (g == kv_heads - 1))
        def _():
            around_copy.wait_recv()
            pass_copy.start()

        keys, values = (
            jnp.concatenate([window[k, g, which] for k in range(back, -1, -1)], axis=0)
            for which in range(2)
        )
        queries, grads = stacked(0, g), stacked(1, g)
        kept = jnp.concatenate([bias[...]] * groups, axis=1)
        scores = dot(keys, queries, 1, 1) * (scaling * math.log2(math.e)) + kept
        peak = jnp.max(scores, axis=0, keepdims=True)
        raised = jnp.exp2(scores - peak)
        weights = raised * (1.0 / jnp.sum(raised, axis=0, keepdims=True))
        weights_bf = weights.astype(jnp.bfloat16)
        attended = dot(values, weights_bf, 0, 0)
        grad_weights = dot(values, grads, 1, 1)
        delta = jnp.sum(weights * grad_weights, axis=0, keepdims=True)
        grad_scores = (weights * (grad_weights - delta)).astype(jnp.bfloat16)
        grad_query = dot(keys, grad_scores, 0, 0) * scaling
        grad_key = dot(grad_scores, queries, 1, 0) * scaling
        grad_value = dot(weights_bf, grads, 1, 0)
        for k in range(1, back + 1):
            at = slice((back - k) * rows, (back - k + 1) * rows)
            part[k - 1, g, 0] = grad_key[at].astype(jnp.bfloat16)
            part[k - 1, g, 1] = grad_value[at].astype(jnp.bfloat16)
        own[g, 0] = grad_key[back * rows :]
        own[g, 1] = grad_value[back * rows :]

        @pl.when(around & (g == per - 1))
        def _():
            around_copy.start()

        for k in range(back, 0, -1):
            detour = around & (g < per) if k == 1 else False
            @pl.when((me - k >= 0) & jnp.logical_not(detour))
            def _():
                g_copy(g, k).start()

        for h in range(groups):
            at = slice(h * HEAD_DIM, (h + 1) * HEAD_DIM)
            to = columns(g * groups + h, HEAD_DIM)
            attbuf[:, to] = attended[:, at].T.astype(jnp.bfloat16)
            dqbuf[:, to] = grad_query[:, at].T.astype(jnp.bfloat16)

    @pl.loop(0, chunks)
    def _(c):
        for n in range(1, back + 1):
            @pl.when(jnp.minimum(total - 1 - me, back) == n)
            def _():
                wait_for(landed.at[pl.ds(0, n), heads(c)], g_recv.at[c])

        for i in range(per):
            g = c * per + i
            sums = own[g]
            for k in range(1, back + 1):
                sums = sums + landed[k - 1, g].astype(jnp.float32)
            dkbuf[:, columns(g, HEAD_DIM)] = sums[0].astype(jnp.bfloat16)
            dvbuf[:, columns(g, HEAD_DIM)] = sums[1].astype(jnp.bfloat16)

    @pl.when(relays)
    def _():
        relay().wait_send()

    @pl.when(passes)
    def _():
        pass_copy.wait_send()

    for k in range(1, back + 1):
        short = edge if k == 1 else jnp.bool_(False)

        @pl.when((me + k < total) & jnp.logical_not(short))
        def _():
            wait_for(window.at[0], kv_send.at[k - 1])

        @pl.when(short)
        def _():
            wait_for(window.at[0, pl.ds(0, last * per)], kv_send.at[k - 1])

        @pl.when(me - k >= 0)
        def _():
            wait_for(part.at[k - 1], g_send.at[k - 1])


def write_out(att, dq, dk, dv, att_hbm, dq_hbm, dk_hbm, dv_hbm, sems):
    pairs = ((att, att_hbm), (dq, dq_hbm), (dk, dk_hbm), (dv, dv_hbm))
    copies = [
        pltpu.make_async_copy(source, target, sems.at[which])
        for which, (source, target) in enumerate(pairs)
    ]
    for copy in copies:
        copy.start()
    for copy in copies:
        copy.wait()


def solution(mesh):
    back = mesh.shape["head"]
    total = mesh.shape["blk"] * back

    def per_device(query, key, value, grad_out, doc_lengths):
        rows, kv_heads = query.shape[0], key.shape[1] // HEAD_DIM
        chunks = kv_heads // math.gcd(kv_heads, HEADS_A_COPY)
        bf, f32 = jnp.bfloat16, jnp.float32
        anywhere = pl.BlockSpec(memory_space=pl.ANY)
        dma = pltpu.SemaphoreType.DMA
        results = pl.pallas_call(
            functools.partial(kernel, back, total),
            out_shape=[
                pltpu.VMEM(query.shape, bf),
                pltpu.VMEM(query.shape, bf),
                pltpu.VMEM(key.shape, bf),
                pltpu.VMEM(key.shape, bf),
            ],
            in_specs=[anywhere] * 5,
            out_specs=[pl.BlockSpec(memory_space=pltpu.VMEM)] * 4,
            scratch_shapes=[
                pltpu.VMEM((back + 1, kv_heads, 2, rows, HEAD_DIM), bf),
                pltpu.VMEM((2, *query.shape), bf),
                pltpu.VMEM((back, kv_heads, 2, rows, HEAD_DIM), bf),
                pltpu.VMEM((back, kv_heads, 2, rows, HEAD_DIM), bf),
                pltpu.VMEM((kv_heads // chunks, 2, rows, HEAD_DIM), bf),
                pltpu.VMEM((kv_heads, 2, rows, HEAD_DIM), f32),
                pltpu.VMEM(((back + 1) * rows, rows), f32),
                pltpu.SMEM(doc_lengths.shape, jnp.int32),
                dma,
                dma,
                dma,
                dma((back,)),
                dma((chunks,)),
                dma,
                dma,
                dma((back,)),
                dma((chunks,)),
                dma,
                dma,
            ],
            compiler_params=pltpu.CompilerParams(collective_id=0, has_side_effects=True),
        )(doc_lengths, query, key, value, grad_out)
        results = [pltpu.with_memory_space_constraint(r, pltpu.VMEM) for r in results]
        return pl.pallas_call(
            write_out,
            out_shape=[
                jax.ShapeDtypeStruct(query.shape, bf),
                jax.ShapeDtypeStruct(query.shape, bf),
                jax.ShapeDtypeStruct(key.shape, bf),
                jax.ShapeDtypeStruct(key.shape, bf),
            ],
            in_specs=[pl.BlockSpec(memory_space=pltpu.VMEM)] * 4,
            out_specs=[anywhere] * 4,
            scratch_shapes=[dma((4,))],
        )(*results)

    split = P(("blk", "head"), None)
    return jax.shard_map(
        per_device,
        mesh=mesh,
        in_specs=(split, split, split, split, P()),
        out_specs=(split, split, split, split),
        check_vma=False,
    )
```

```python
import functools
import math

import jax
import jax.numpy as jnp
from jax import lax
from jax.experimental import pallas as pl
from jax.experimental.pallas import tpu as pltpu
from jax.sharding import PartitionSpec as P

HEAD_DIM = 128
EXCLUDED = -1e30
HEADS_A_COPY = 2
MESH = pl.DeviceIdType.MESH


def kernel(
    back, total, lens_hbm, q_hbm, k_hbm, v_hbm, do_hbm, attbuf, dqbuf, dkbuf, dvbuf,
    window, qbuf, part, landed, passing, own, bias, lens,
    lens_in, kv_in, q_in, kv_send, kv_recv, edge_recv, relay_send, g_send, g_recv, pass_recv, pass_send,
):
    rows = q_hbm.shape[0]
    kv_heads = k_hbm.shape[1] // HEAD_DIM
    groups = q_hbm.shape[1] // k_hbm.shape[1]
    span = (back + 1) * rows
    scaling = HEAD_DIM ** (-0.5)
    chunks = g_recv.shape[0]
    per = kv_heads // chunks
    last = chunks - 1
    me = lax.axis_index("blk") * back + lax.axis_index("head")
    place = me % (2 * back)
    edge = (place == 2 * back - 1) & (me + back < total) & (back == 2)
    relays = (place == 1) & (me > back) & (back == 2)
    around = (place == 0) & (me > back) & (back == 2)
    passes = (place == 2) & (me + back < total) & (back == 2)

    def device(number):
        return {"blk": number // back, "head": number % back}

    def columns(g, size):
        return pl.ds(pl.multiple_of(g * size, size), size)

    def heads(c):
        return pl.ds(c * per, per)

    def kv_load(g, which):
        return pltpu.make_async_copy(
            (k_hbm, v_hbm)[which].at[:, columns(g, HEAD_DIM)],
            window.at[0, g, which],
            kv_in,
        )

    q_load = pltpu.make_async_copy(q_hbm, qbuf.at[0], q_in)
    do_load = pltpu.make_async_copy(do_hbm, qbuf.at[1], q_in)

    def wait_for(landing, sem):
        pltpu.make_async_copy(landing, landing, sem).wait()

    def kv_copy(c, k):
        return pltpu.make_async_remote_copy(
            src_ref=window.at[0, heads(c)],
            dst_ref=window.at[k, heads(c)],
            send_sem=kv_send.at[k - 1],
            recv_sem=kv_recv.at[c],
            device_id=device(me + k),
            device_id_type=MESH,
        )

    def first_copy(g, which, k):
        return pltpu.make_async_remote_copy(
            src_ref=(k_hbm, v_hbm)[which].at[:, columns(g, HEAD_DIM)],
            dst_ref=window.at[k, g, which],
            send_sem=kv_send.at[k - 1],
            recv_sem=kv_recv.at[0],
            device_id=device(me + k),
            device_id_type=MESH,
        )

    edge_copy = pltpu.make_async_remote_copy(
        src_ref=window.at[0, heads(last)],
        dst_ref=window.at[back, heads(last)],
        send_sem=kv_send.at[back - 1],
        recv_sem=edge_recv,
        device_id=device(me + back),
        device_id_type=MESH,
    )

    def relay():
        return pltpu.make_async_remote_copy(
            src_ref=window.at[back, heads(last)],
            dst_ref=window.at[1, heads(last)],
            send_sem=relay_send,
            recv_sem=kv_recv.at[last],
            device_id=device(me - 1),
            device_id_type=MESH,
        )

    def g_copy(g, k):
        return pltpu.make_async_remote_copy(
            src_ref=part.at[k - 1, g],
            dst_ref=landed.at[k - 1, g],
            send_sem=g_send.at[k - 1],
            recv_sem=g_recv.at[g // per],
            device_id=device(me - k),
            device_id_type=MESH,
        )

    barrier = pltpu.get_barrier_semaphore()
    for k in range(1, back + 1):
        @pl.when(me - k >= 0)
        def _():
            pl.semaphore_signal(barrier, inc=1, device_id=device(me - k), device_id_type=MESH)

    around_copy = pltpu.make_async_remote_copy(
        src_ref=part.at[0, heads(0)],
        dst_ref=passing,
        send_sem=g_send.at[0],
        recv_sem=pass_recv,
        device_id=device(me - back),
        device_id_type=MESH,
    )
    pass_copy = pltpu.make_async_remote_copy(
        src_ref=passing,
        dst_ref=landed.at[0, heads(0)],
        send_sem=pass_send,
        recv_sem=g_recv.at[0],
        device_id=device(me + 1),
        device_id_type=MESH,
    )

    eager = place == 1

    def load():
        @pl.loop(0, kv_heads)
        def _(g):
            kv_load(g, 0).start()
            kv_load(g, 1).start()

    @pl.when(jnp.logical_not(eager))
    def _():
        load()

    @pl.when(me < total - 1)
    def _():
        pl.semaphore_wait(barrier, jnp.minimum(total - 1 - me, back))

    @pl.when(eager)
    def _():
        for g in range(per):
            for which in range(2):
                first_copy(g, which, 1).start()

        load()

    lens_load = pltpu.make_async_copy(lens_hbm, lens, lens_in)
    lens_load.start()
    wait_for(window.at[0], kv_in)

    @pl.when(edge)
    def _():
        kv_copy(0, 1).start()
        edge_copy.start()
        kv_copy(0, back).start()

    @pl.loop(edge.astype(jnp.int32), chunks - edge.astype(jnp.int32))
    def _(c):
        for k in range(1, back + 1):
            later = (relays & (c == last)) | (eager & (c == 0)) if k == 1 else False
            @pl.when((me + k < total) & jnp.logical_not(later))
            def _():
                kv_copy(c, k).start()

    q_load.start()
    do_load.start()

    for k in range(1, back + 1):
        @pl.when(me - k < 0)
        def _():
            window[k] = jnp.zeros((kv_heads, 2, rows, HEAD_DIM), jnp.bfloat16)

        @pl.when(me + k >= total)
        def _():
            landed[k - 1] = jnp.zeros((kv_heads, 2, rows, HEAD_DIM), jnp.bfloat16)

    lens_load.wait()
    query_pos = me * rows + lax.broadcasted_iota(jnp.int32, (1, rows), 1)

    def latest(d, carry):
        start, first = carry
        return start + lens[d], jnp.where(query_pos >= start, start, first)

    _, first = lax.fori_loop(
        0, lens.shape[0], latest, (jnp.int32(0), jnp.zeros((1, rows), jnp.int32))
    )
    key_pos = (me - back) * rows + lax.broadcasted_iota(jnp.int32, (span, rows), 0)
    bias[...] = jnp.where((key_pos <= query_pos) & (key_pos >= first), 0.0, EXCLUDED)

    def dot(a, b, a_dim, b_dim):
        return lax.dot_general(
            a, b, (((a_dim,), (b_dim,)), ((), ())), preferred_element_type=jnp.float32
        )

    def stacked(which, g):
        return jnp.concatenate(
            [qbuf[which, :, columns(g * groups + h, HEAD_DIM)] for h in range(groups)], axis=0
        )

    wait_for(qbuf, q_in)

    @pl.loop(0, kv_heads)
    def _(g):
        @pl.when(g % per == 0)
        def _():
            early = relays & (g == last * per)
            for n in range(1, back + 1):
                @pl.when((jnp.minimum(me, back) - early.astype(jnp.int32)) == n)
                def _():
                    wait_for(window.at[pl.ds(1, n), heads(g // per)], kv_recv.at[g // per])

        @pl.when(relays & (g == 0))
        def _():
            edge_copy.wait_recv()
            relay().start()
            kv_copy(last, 1).start()

        @pl.when(passes & (g == kv_heads - 1))
        def _():
            around_copy.wait_recv()
            pass_copy.start()

        keys, values = (
            jnp.concatenate([window[k, g, which] for k in range(back, -1, -1)], axis=0)
            for which in range(2)
        )
        queries, grads = stacked(0, g), stacked(1, g)
        kept = jnp.concatenate([bias[...]] * groups, axis=1)
        scores = dot(keys, queries, 1, 1) * (scaling * math.log2(math.e)) + kept
        peak = jnp.max(scores, axis=0, keepdims=True)
        raised = jnp.exp2(scores - peak)
        weights = raised * (1.0 / jnp.sum(raised, axis=0, keepdims=True))
        weights_bf = weights.astype(jnp.bfloat16)
        attended = dot(values, weights_bf, 0, 0)
        grad_weights = dot(values, grads, 1, 1)
        delta = jnp.sum(weights * grad_weights, axis=0, keepdims=True)
        grad_scores = (weights * (grad_weights - delta)).astype(jnp.bfloat16)
        grad_query = dot(keys, grad_scores, 0, 0) * scaling
        grad_key = dot(grad_scores, queries, 1, 0) * scaling
        grad_value = dot(weights_bf, grads, 1, 0)
        for k in range(1, back + 1):
            at = slice((back - k) * rows, (back - k + 1) * rows)
            part[k - 1, g, 0] = grad_key[at].astype(jnp.bfloat16)
            part[k - 1, g, 1] = grad_value[at].astype(jnp.bfloat16)
        own[g, 0] = grad_key[back * rows :]
        own[g, 1] = grad_value[back * rows :]

        @pl.when(around & (g == per - 1))
        def _():
            around_copy.start()

        for k in range(back, 0, -1):
            detour = around & (g < per) if k == 1 else False
            @pl.when((me - k >= 0) & jnp.logical_not(detour))
            def _():
                g_copy(g, k).start()

        for h in range(groups):
            at = slice(h * HEAD_DIM, (h + 1) * HEAD_DIM)
            to = columns(g * groups + h, HEAD_DIM)
            attbuf[:, to] = attended[:, at].T.astype(jnp.bfloat16)
            dqbuf[:, to] = grad_query[:, at].T.astype(jnp.bfloat16)

    @pl.loop(0, chunks)
    def _(c):
        for n in range(1, back + 1):
            @pl.when(jnp.minimum(total - 1 - me, back) == n)
            def _():
                wait_for(landed.at[pl.ds(0, n), heads(c)], g_recv.at[c])

        for i in range(per):
            g = c * per + i
            sums = own[g]
            for k in range(1, back + 1):
                sums = sums + landed[k - 1, g].astype(jnp.float32)
            dkbuf[:, columns(g, HEAD_DIM)] = sums[0].astype(jnp.bfloat16)
            dvbuf[:, columns(g, HEAD_DIM)] = sums[1].astype(jnp.bfloat16)

    @pl.when(relays)
    def _():
        relay().wait_send()

    @pl.when(passes)
    def _():
        pass_copy.wait_send()

    for k in range(1, back + 1):
        short = edge if k == 1 else jnp.bool_(False)

        @pl.when((me + k < total) & jnp.logical_not(short))
        def _():
            wait_for(window.at[0], kv_send.at[k - 1])

        @pl.when(short)
        def _():
            wait_for(window.at[0, pl.ds(0, last * per)], kv_send.at[k - 1])

        @pl.when(me - k >= 0)
        def _():
            wait_for(part.at[k - 1], g_send.at[k - 1])


def write_out(att, dq, dk, dv, att_hbm, dq_hbm, dk_hbm, dv_hbm, sems):
    pairs = ((att, att_hbm), (dq, dq_hbm), (dk, dk_hbm), (dv, dv_hbm))
    copies = [
        pltpu.make_async_copy(source, target, sems.at[which])
        for which, (source, target) in enumerate(pairs)
    ]
    for copy in copies:
        copy.start()
    for copy in copies:
        copy.wait()


def solution(mesh):
    back = mesh.shape["head"]
    total = mesh.shape["blk"] * back

    def per_device(query, key, value, grad_out, doc_lengths):
        rows, kv_heads = query.shape[0], key.shape[1] // HEAD_DIM
        chunks = kv_heads // math.gcd(kv_heads, HEADS_A_COPY)
        bf, f32 = jnp.bfloat16, jnp.float32
        anywhere = pl.BlockSpec(memory_space=pl.ANY)
        dma = pltpu.SemaphoreType.DMA
        results = pl.pallas_call(
            functools.partial(kernel, back, total),
            out_shape=[
                pltpu.VMEM(query.shape, bf),
                pltpu.VMEM(query.shape, bf),
                pltpu.VMEM(key.shape, bf),
                pltpu.VMEM(key.shape, bf),
            ],
            in_specs=[anywhere] * 5,
            out_specs=[pl.BlockSpec(memory_space=pltpu.VMEM)] * 4,
            scratch_shapes=[
                pltpu.VMEM((back + 1, kv_heads, 2, rows, HEAD_DIM), bf),
                pltpu.VMEM((2, *query.shape), bf),
                pltpu.VMEM((back, kv_heads, 2, rows, HEAD_DIM), bf),
                pltpu.VMEM((back, kv_heads, 2, rows, HEAD_DIM), bf),
                pltpu.VMEM((kv_heads // chunks, 2, rows, HEAD_DIM), bf),
                pltpu.VMEM((kv_heads, 2, rows, HEAD_DIM), f32),
                pltpu.VMEM(((back + 1) * rows, rows), f32),
                pltpu.SMEM(doc_lengths.shape, jnp.int32),
                dma,
                dma,
                dma,
                dma((back,)),
                dma((chunks,)),
                dma,
                dma,
                dma((back,)),
                dma((chunks,)),
                dma,
                dma,
            ],
            compiler_params=pltpu.CompilerParams(collective_id=0, has_side_effects=True),
        )(doc_lengths, query, key, value, grad_out)
        results = [pltpu.with_memory_space_constraint(r, pltpu.VMEM) for r in results]
        return pl.pallas_call(
            write_out,
            out_shape=[
                jax.ShapeDtypeStruct(query.shape, bf),
                jax.ShapeDtypeStruct(query.shape, bf),
                jax.ShapeDtypeStruct(key.shape, bf),
                jax.ShapeDtypeStruct(key.shape, bf),
            ],
            in_specs=[pl.BlockSpec(memory_space=pltpu.VMEM)] * 4,
            out_specs=[anywhere] * 4,
            scratch_shapes=[dma((4,))],
        )(*results)

    split = P(("blk", "head"), None)
    return jax.shard_map(
        per_device,
        mesh=mesh,
        in_specs=(split, split, split, split, P()),
        out_specs=(split, split, split, split),
        check_vma=False,
    )
```

```python
import functools
import math

import jax
import jax.numpy as jnp
from jax import lax
from jax.experimental import pallas as pl
from jax.experimental.pallas import tpu as pltpu
from jax.sharding import PartitionSpec as P

HEAD_DIM = 128
EXCLUDED = -1e30
HEADS_A_COPY = 2
MESH = pl.DeviceIdType.MESH


def kernel(
    back, total, lens_hbm, q_hbm, k_hbm, v_hbm, do_hbm, attbuf, dqbuf, dkbuf, dvbuf,
    window, qbuf, part, landed, passing, own, bias, lens,
    lens_in, kv_in, kv_send, kv_recv, detour_recv, detour_send, g_send, g_recv,
):
    rows = q_hbm.shape[0]
    kv_heads = k_hbm.shape[1] // HEAD_DIM
    groups = q_hbm.shape[1] // k_hbm.shape[1]
    span = (back + 1) * rows
    scaling = HEAD_DIM ** (-0.5)
    chunks = g_recv.shape[0]
    per = kv_heads // chunks
    last = chunks - 1
    me = lax.axis_index("blk") * back + lax.axis_index("head")
    place = me % (2 * back)
    edge = (place == 2 * back - 1) & (me + back < total) & (back == 2)
    relays = (place == 1) & (me > back) & (back == 2)
    around = (place == 0) & (me > back) & (back == 2)
    passes = (place == 2) & (me + back < total) & (back == 2)

    def device(number):
        return {"blk": number // back, "head": number % back}

    def columns(g, size):
        return pl.ds(pl.multiple_of(g * size, size), size)

    def heads(c):
        return pl.ds(c * per, per)

    def kv_load(g, which):
        return pltpu.make_async_copy(
            (k_hbm, v_hbm)[which].at[:, columns(g, HEAD_DIM)],
            window.at[0, g, which],
            kv_in,
        )

    q_load = pltpu.make_async_copy(q_hbm, qbuf.at[0], kv_in)
    do_load = pltpu.make_async_copy(do_hbm, qbuf.at[1], kv_in)

    def wait_for(landing, sem):
        pltpu.make_async_copy(landing, landing, sem).wait()

    def kv_copy(c, k):
        return pltpu.make_async_remote_copy(
            src_ref=window.at[0, heads(c)],
            dst_ref=window.at[k, heads(c)],
            send_sem=kv_send.at[k - 1],
            recv_sem=kv_recv.at[c],
            device_id=device(me + k),
            device_id_type=MESH,
        )

    def first_copy(g, which, k):
        return pltpu.make_async_remote_copy(
            src_ref=(k_hbm, v_hbm)[which].at[:, columns(g, HEAD_DIM)],
            dst_ref=window.at[k, g, which],
            send_sem=kv_send.at[k - 1],
            recv_sem=kv_recv.at[0],
            device_id=device(me + k),
            device_id_type=MESH,
        )

    edge_copy = pltpu.make_async_remote_copy(
        src_ref=window.at[0, heads(last)],
        dst_ref=window.at[back, heads(last)],
        send_sem=kv_send.at[back - 1],
        recv_sem=detour_recv,
        device_id=device(me + back),
        device_id_type=MESH,
    )

    def relay():
        return pltpu.make_async_remote_copy(
            src_ref=window.at[back, heads(last)],
            dst_ref=window.at[1, heads(last)],
            send_sem=detour_send,
            recv_sem=kv_recv.at[last],
            device_id=device(me - 1),
            device_id_type=MESH,
        )

    def g_copy(g, k):
        return pltpu.make_async_remote_copy(
            src_ref=part.at[k - 1, g],
            dst_ref=landed.at[k - 1, g],
            send_sem=g_send.at[k - 1],
            recv_sem=g_recv.at[g // per],
            device_id=device(me - k),
            device_id_type=MESH,
        )

    barrier = pltpu.get_barrier_semaphore()
    for k in range(1, back + 1):
        @pl.when(me - k >= 0)
        def _():
            pl.semaphore_signal(barrier, inc=1, device_id=device(me - k), device_id_type=MESH)

    around_copy = pltpu.make_async_remote_copy(
        src_ref=part.at[0, heads(0)],
        dst_ref=passing,
        send_sem=g_send.at[0],
        recv_sem=detour_recv,
        device_id=device(me - back),
        device_id_type=MESH,
    )
    pass_copy = pltpu.make_async_remote_copy(
        src_ref=passing,
        dst_ref=landed.at[0, heads(0)],
        send_sem=detour_send,
        recv_sem=g_recv.at[0],
        device_id=device(me + 1),
        device_id_type=MESH,
    )

    eager = place == 1

    def load():
        @pl.loop(0, kv_heads)
        def _(g):
            kv_load(g, 0).start()
            kv_load(g, 1).start()

    @pl.when(jnp.logical_not(eager))
    def _():
        load()

    @pl.when(me < total - 1)
    def _():
        pl.semaphore_wait(barrier, jnp.minimum(total - 1 - me, back))

    @pl.when(eager)
    def _():
        for g in range(per):
            for which in range(2):
                first_copy(g, which, 1).start()

        load()

    lens_load = pltpu.make_async_copy(lens_hbm, lens, lens_in)
    lens_load.start()
    wait_for(window.at[0], kv_in)

    @pl.when(edge)
    def _():
        kv_copy(0, 1).start()
        edge_copy.start()
        kv_copy(0, back).start()

    @pl.loop(edge.astype(jnp.int32), chunks - edge.astype(jnp.int32))
    def _(c):
        for k in range(1, back + 1):
            later = (relays & (c == last)) | (eager & (c == 0)) if k == 1 else False
            @pl.when((me + k < total) & jnp.logical_not(later))
            def _():
                kv_copy(c, k).start()

    q_load.start()
    do_load.start()

    for k in range(1, back + 1):
        @pl.when(me - k < 0)
        def _():
            window[k] = jnp.zeros((kv_heads, 2, rows, HEAD_DIM), jnp.bfloat16)

        @pl.when(me + k >= total)
        def _():
            landed[k - 1] = jnp.zeros((kv_heads, 2, rows, HEAD_DIM), jnp.bfloat16)

    lens_load.wait()
    query_pos = me * rows + lax.broadcasted_iota(jnp.int32, (1, rows), 1)

    def latest(d, carry):
        start, first = carry
        return start + lens[d], jnp.where(query_pos >= start, start, first)

    _, first = lax.fori_loop(
        0, lens.shape[0], latest, (jnp.int32(0), jnp.zeros((1, rows), jnp.int32))
    )
    key_pos = (me - back) * rows + lax.broadcasted_iota(jnp.int32, (span, rows), 0)
    bias[...] = jnp.where((key_pos <= query_pos) & (key_pos >= first), 0.0, EXCLUDED)

    def dot(a, b, a_dim, b_dim):
        return lax.dot_general(
            a, b, (((a_dim,), (b_dim,)), ((), ())), preferred_element_type=jnp.float32
        )

    def stacked(which, g):
        return jnp.concatenate(
            [qbuf[which, :, columns(g * groups + h, HEAD_DIM)] for h in range(groups)], axis=0
        )

    wait_for(qbuf, kv_in)

    @pl.loop(0, kv_heads)
    def _(g):
        @pl.when(g % per == 0)
        def _():
            early = relays & (g == last * per)
            for n in range(1, back + 1):
                @pl.when((jnp.minimum(me, back) - early.astype(jnp.int32)) == n)
                def _():
                    wait_for(window.at[pl.ds(1, n), heads(g // per)], kv_recv.at[g // per])

        @pl.when(relays & (g == 0))
        def _():
            edge_copy.wait_recv()
            relay().start()
            kv_copy(last, 1).start()

        @pl.when(passes & (g == kv_heads - 1))
        def _():
            around_copy.wait_recv()
            pass_copy.start()

        keys, values = (
            jnp.concatenate([window[k, g, which] for k in range(back, -1, -1)], axis=0)
            for which in range(2)
        )
        queries, grads = stacked(0, g), stacked(1, g)
        kept = jnp.concatenate([bias[...]] * groups, axis=1)
        scores = dot(keys, queries, 1, 1) * (scaling * math.log2(math.e)) + kept
        peak = jnp.max(scores, axis=0, keepdims=True)
        raised = jnp.exp2(scores - peak)
        weights = raised * (1.0 / jnp.sum(raised, axis=0, keepdims=True))
        weights_bf = weights.astype(jnp.bfloat16)
        attended = dot(values, weights_bf, 0, 0)
        grad_weights = dot(values, grads, 1, 1)
        delta = jnp.sum(weights * grad_weights, axis=0, keepdims=True)
        grad_scores = (weights * (grad_weights - delta)).astype(jnp.bfloat16)
        grad_query = dot(keys, grad_scores, 0, 0) * scaling
        grad_key = dot(grad_scores, queries, 1, 0) * scaling
        grad_value = dot(weights_bf, grads, 1, 0)
        for k in range(1, back + 1):
            at = slice((back - k) * rows, (back - k + 1) * rows)
            part[k - 1, g, 0] = grad_key[at].astype(jnp.bfloat16)
            part[k - 1, g, 1] = grad_value[at].astype(jnp.bfloat16)
        own[g, 0] = grad_key[back * rows :]
        own[g, 1] = grad_value[back * rows :]

        @pl.when(around & (g == per - 1))
        def _():
            around_copy.start()

        for k in range(back, 0, -1):
            detour = around & (g < per) if k == 1 else False
            @pl.when((me - k >= 0) & jnp.logical_not(detour))
            def _():
                g_copy(g, k).start()

        for h in range(groups):
            at = slice(h * HEAD_DIM, (h + 1) * HEAD_DIM)
            to = columns(g * groups + h, HEAD_DIM)
            attbuf[:, to] = attended[:, at].T.astype(jnp.bfloat16)
            dqbuf[:, to] = grad_query[:, at].T.astype(jnp.bfloat16)

    def total_up(c):
        for n in range(1, back + 1):
            @pl.when(jnp.minimum(total - 1 - me, back) == n)
            def _():
                wait_for(landed.at[pl.ds(0, n), heads(c)], g_recv.at[c])

        for i in range(per):
            g = c * per + i
            sums = own[g]
            for k in range(1, back + 1):
                sums = sums + landed[k - 1, g].astype(jnp.float32)
            dkbuf[:, columns(g, HEAD_DIM)] = sums[0].astype(jnp.bfloat16)
            dvbuf[:, columns(g, HEAD_DIM)] = sums[1].astype(jnp.bfloat16)

    @pl.loop(0, last)
    def _(c):
        total_up(c)

    @pl.when(relays)
    def _():
        relay().wait_send()

    @pl.when(passes)
    def _():
        pass_copy.wait_send()

    for k in range(1, back + 1):
        short = edge if k == 1 else jnp.bool_(False)

        @pl.when((me + k < total) & jnp.logical_not(short))
        def _():
            wait_for(window.at[0], kv_send.at[k - 1])

        @pl.when(short)
        def _():
            wait_for(window.at[0, pl.ds(0, last * per)], kv_send.at[k - 1])

        @pl.when(me - k >= 0)
        def _():
            wait_for(part.at[k - 1], g_send.at[k - 1])

    total_up(last)


def write_out(att, dq, dk, dv, att_hbm, dq_hbm, dk_hbm, dv_hbm, sems):
    pairs = ((att, att_hbm), (dq, dq_hbm), (dk, dk_hbm), (dv, dv_hbm))
    copies = [
        pltpu.make_async_copy(source, target, sems.at[which])
        for which, (source, target) in enumerate(pairs)
    ]
    for copy in copies:
        copy.start()
    for copy in copies:
        copy.wait()


def solution(mesh):
    back = mesh.shape["head"]
    total = mesh.shape["blk"] * back

    def per_device(query, key, value, grad_out, doc_lengths):
        rows, kv_heads = query.shape[0], key.shape[1] // HEAD_DIM
        chunks = kv_heads // math.gcd(kv_heads, HEADS_A_COPY)
        bf, f32 = jnp.bfloat16, jnp.float32
        anywhere = pl.BlockSpec(memory_space=pl.ANY)
        dma = pltpu.SemaphoreType.DMA
        results = pl.pallas_call(
            functools.partial(kernel, back, total),
            out_shape=[
                pltpu.VMEM(query.shape, bf),
                pltpu.VMEM(query.shape, bf),
                pltpu.VMEM(key.shape, bf),
                pltpu.VMEM(key.shape, bf),
            ],
            in_specs=[anywhere] * 5,
            out_specs=[pl.BlockSpec(memory_space=pltpu.VMEM)] * 4,
            scratch_shapes=[
                pltpu.VMEM((back + 1, kv_heads, 2, rows, HEAD_DIM), bf),
                pltpu.VMEM((2, *query.shape), bf),
                pltpu.VMEM((back, kv_heads, 2, rows, HEAD_DIM), bf),
                pltpu.VMEM((back, kv_heads, 2, rows, HEAD_DIM), bf),
                pltpu.VMEM((kv_heads // chunks, 2, rows, HEAD_DIM), bf),
                pltpu.VMEM((kv_heads, 2, rows, HEAD_DIM), f32),
                pltpu.VMEM(((back + 1) * rows, rows), f32),
                pltpu.SMEM(doc_lengths.shape, jnp.int32),
                dma,
                dma,
                dma((back,)),
                dma((chunks,)),
                dma,
                dma,
                dma((back,)),
                dma((chunks,)),
            ],
            compiler_params=pltpu.CompilerParams(collective_id=0, has_side_effects=True),
        )(doc_lengths, query, key, value, grad_out)
        results = [pltpu.with_memory_space_constraint(r, pltpu.VMEM) for r in results]
        return pl.pallas_call(
            write_out,
            out_shape=[
                jax.ShapeDtypeStruct(query.shape, bf),
                jax.ShapeDtypeStruct(query.shape, bf),
                jax.ShapeDtypeStruct(key.shape, bf),
                jax.ShapeDtypeStruct(key.shape, bf),
            ],
            in_specs=[pl.BlockSpec(memory_space=pltpu.VMEM)] * 4,
            out_specs=[anywhere] * 4,
            scratch_shapes=[dma((4,))],
        )(*results)

    split = P(("blk", "head"), None)
    return jax.shard_map(
        per_device,
        mesh=mesh,
        in_specs=(split, split, split, split, P()),
        out_specs=(split, split, split, split),
        check_vma=False,
    )
```

```python
import functools
import math

import jax
import jax.numpy as jnp
from jax import lax
from jax.experimental import pallas as pl
from jax.experimental.pallas import tpu as pltpu
from jax.sharding import PartitionSpec as P

HEAD_DIM = 128
EXCLUDED = -1e30
HEADS_A_COPY = 2
MESH = pl.DeviceIdType.MESH


def kernel(
    back, total, lens_hbm, q_hbm, k_hbm, v_hbm, do_hbm, attbuf, dqbuf, dkbuf, dvbuf,
    window, qbuf, part, landed, passing, own, bias, lens,
    lens_in, kv_in, kv_send, kv_recv, detour_recv, detour_send, g_send, g_recv,
):
    rows = q_hbm.shape[0]
    kv_heads = k_hbm.shape[1] // HEAD_DIM
    groups = q_hbm.shape[1] // k_hbm.shape[1]
    span = (back + 1) * rows
    scaling = HEAD_DIM ** (-0.5)
    chunks = g_recv.shape[0]
    per = kv_heads // chunks
    last = chunks - 1
    me = lax.axis_index("blk") * back + lax.axis_index("head")
    place = me % (2 * back)
    edge = (place == 2 * back - 1) & (me + back < total) & (back == 2)
    relays = (place == 1) & (me > back) & (back == 2)
    around = (place == 0) & (me > back) & (back == 2)
    passes = (place == 2) & (me + back < total) & (back == 2)

    def device(number):
        return {"blk": number // back, "head": number % back}

    def columns(g, size):
        return pl.ds(pl.multiple_of(g * size, size), size)

    def heads(c):
        return pl.ds(c * per, per)

    def kv_load(g, which):
        return pltpu.make_async_copy(
            (k_hbm, v_hbm)[which].at[:, columns(g, HEAD_DIM)],
            window.at[0, g, which],
            kv_in,
        )

    q_load = pltpu.make_async_copy(q_hbm, qbuf.at[0], kv_in)
    do_load = pltpu.make_async_copy(do_hbm, qbuf.at[1], kv_in)

    def wait_for(landing, sem):
        pltpu.make_async_copy(landing, landing, sem).wait()

    def kv_copy(c, k):
        return pltpu.make_async_remote_copy(
            src_ref=window.at[0, heads(c)],
            dst_ref=window.at[k, heads(c)],
            send_sem=kv_send.at[k - 1],
            recv_sem=kv_recv.at[c],
            device_id=device(me + k),
            device_id_type=MESH,
        )

    def first_copy(g, which, k):
        return pltpu.make_async_remote_copy(
            src_ref=(k_hbm, v_hbm)[which].at[:, columns(g, HEAD_DIM)],
            dst_ref=window.at[k, g, which],
            send_sem=kv_send.at[k - 1],
            recv_sem=kv_recv.at[0],
            device_id=device(me + k),
            device_id_type=MESH,
        )

    edge_copy = pltpu.make_async_remote_copy(
        src_ref=window.at[0, heads(last)],
        dst_ref=window.at[back, heads(last)],
        send_sem=kv_send.at[back - 1],
        recv_sem=detour_recv,
        device_id=device(me + back),
        device_id_type=MESH,
    )

    def relay():
        return pltpu.make_async_remote_copy(
            src_ref=window.at[back, heads(last)],
            dst_ref=window.at[1, heads(last)],
            send_sem=detour_send,
            recv_sem=kv_recv.at[last],
            device_id=device(me - 1),
            device_id_type=MESH,
        )

    def g_copy(g, k):
        return pltpu.make_async_remote_copy(
            src_ref=part.at[k - 1, g],
            dst_ref=landed.at[k - 1, g],
            send_sem=g_send.at[k - 1],
            recv_sem=g_recv.at[g // per],
            device_id=device(me - k),
            device_id_type=MESH,
        )

    barrier = pltpu.get_barrier_semaphore()
    for k in range(1, back + 1):
        @pl.when(me - k >= 0)
        def _():
            pl.semaphore_signal(barrier, inc=1, device_id=device(me - k), device_id_type=MESH)

    around_copy = pltpu.make_async_remote_copy(
        src_ref=part.at[0, heads(0)],
        dst_ref=passing,
        send_sem=g_send.at[0],
        recv_sem=detour_recv,
        device_id=device(me - back),
        device_id_type=MESH,
    )
    pass_copy = pltpu.make_async_remote_copy(
        src_ref=passing,
        dst_ref=landed.at[0, heads(0)],
        send_sem=detour_send,
        recv_sem=g_recv.at[0],
        device_id=device(me + 1),
        device_id_type=MESH,
    )

    eager = place == 1

    def load():
        @pl.loop(0, kv_heads)
        def _(g):
            kv_load(g, 0).start()
            kv_load(g, 1).start()

    @pl.when(jnp.logical_not(eager))
    def _():
        load()

    @pl.when(me < total - 1)
    def _():
        pl.semaphore_wait(barrier, jnp.minimum(total - 1 - me, back))

    @pl.when(eager)
    def _():
        for g in range(per):
            for which in range(2):
                first_copy(g, which, 1).start()

        load()

    lens_load = pltpu.make_async_copy(lens_hbm, lens, lens_in)
    lens_load.start()
    wait_for(window.at[0], kv_in)

    @pl.when(edge)
    def _():
        kv_copy(0, 1).start()
        edge_copy.start()
        kv_copy(0, back).start()

    @pl.loop(edge.astype(jnp.int32), chunks - edge.astype(jnp.int32))
    def _(c):
        for k in range(1, back + 1):
            later = (relays & (c == last)) | (eager & (c == 0)) if k == 1 else False
            @pl.when((me + k < total) & jnp.logical_not(later))
            def _():
                kv_copy(c, k).start()

    q_load.start()
    do_load.start()

    for k in range(1, back + 1):
        @pl.when(me - k < 0)
        def _():
            window[k] = jnp.zeros((kv_heads, 2, rows, HEAD_DIM), jnp.bfloat16)

        @pl.when(me + k >= total)
        def _():
            landed[k - 1] = jnp.zeros((kv_heads, 2, rows, HEAD_DIM), jnp.bfloat16)

    lens_load.wait()
    query_pos = me * rows + lax.broadcasted_iota(jnp.int32, (1, rows), 1)

    def latest(d, carry):
        start, first = carry
        return start + lens[d], jnp.where(query_pos >= start, start, first)

    _, first = lax.fori_loop(
        0, lens.shape[0], latest, (jnp.int32(0), jnp.zeros((1, rows), jnp.int32))
    )
    key_pos = (me - back) * rows + lax.broadcasted_iota(jnp.int32, (span, rows), 0)
    bias[...] = jnp.where((key_pos <= query_pos) & (key_pos >= first), 0.0, EXCLUDED)

    def dot(a, b, a_dim, b_dim):
        return lax.dot_general(
            a, b, (((a_dim,), (b_dim,)), ((), ())), preferred_element_type=jnp.float32
        )

    def stacked(which, g):
        return jnp.concatenate(
            [qbuf[which, :, columns(g * groups + h, HEAD_DIM)] for h in range(groups)], axis=0
        )

    wait_for(qbuf, kv_in)

    @pl.loop(0, kv_heads)
    def _(g):
        @pl.when(g % per == 0)
        def _():
            early = relays & (g == last * per)
            for n in range(1, back + 1):
                @pl.when((jnp.minimum(me, back) - early.astype(jnp.int32)) == n)
                def _():
                    wait_for(window.at[pl.ds(1, n), heads(g // per)], kv_recv.at[g // per])

        @pl.when(relays & (g == 0))
        def _():
            edge_copy.wait_recv()
            relay().start()
            kv_copy(last, 1).start()

        @pl.when(passes & (g == kv_heads - 2))
        def _():
            around_copy.wait_recv()
            pass_copy.start()

        keys, values = (
            jnp.concatenate([window[k, g, which] for k in range(back, -1, -1)], axis=0)
            for which in range(2)
        )
        queries, grads = stacked(0, g), stacked(1, g)
        kept = jnp.concatenate([bias[...]] * groups, axis=1)
        scores = dot(keys, queries, 1, 1) * (scaling * math.log2(math.e)) + kept
        peak = jnp.max(scores, axis=0, keepdims=True)
        raised = jnp.exp2(scores - peak)
        weights = raised * (1.0 / jnp.sum(raised, axis=0, keepdims=True))
        weights_bf = weights.astype(jnp.bfloat16)
        attended = dot(values, weights_bf, 0, 0)
        grad_weights = dot(values, grads, 1, 1)
        delta = jnp.sum(weights * grad_weights, axis=0, keepdims=True)
        grad_scores = (weights * (grad_weights - delta)).astype(jnp.bfloat16)
        grad_query = dot(keys, grad_scores, 0, 0) * scaling
        grad_key = dot(grad_scores, queries, 1, 0) * scaling
        grad_value = dot(weights_bf, grads, 1, 0)
        for k in range(1, back + 1):
            at = slice((back - k) * rows, (back - k + 1) * rows)
            part[k - 1, g, 0] = grad_key[at].astype(jnp.bfloat16)
            part[k - 1, g, 1] = grad_value[at].astype(jnp.bfloat16)
        own[g, 0] = grad_key[back * rows :]
        own[g, 1] = grad_value[back * rows :]

        @pl.when(around & (g == per - 1))
        def _():
            around_copy.start()

        for k in range(back, 0, -1):
            detour = around & (g < per) if k == 1 else False
            @pl.when((me - k >= 0) & jnp.logical_not(detour))
            def _():
                g_copy(g, k).start()

        for h in range(groups):
            at = slice(h * HEAD_DIM, (h + 1) * HEAD_DIM)
            to = columns(g * groups + h, HEAD_DIM)
            attbuf[:, to] = attended[:, at].T.astype(jnp.bfloat16)
            dqbuf[:, to] = grad_query[:, at].T.astype(jnp.bfloat16)

    def total_up(c):
        for n in range(1, back + 1):
            @pl.when(jnp.minimum(total - 1 - me, back) == n)
            def _():
                wait_for(landed.at[pl.ds(0, n), heads(c)], g_recv.at[c])

        for i in range(per):
            g = c * per + i
            sums = own[g]
            for k in range(1, back + 1):
                sums = sums + landed[k - 1, g].astype(jnp.float32)
            dkbuf[:, columns(g, HEAD_DIM)] = sums[0].astype(jnp.bfloat16)
            dvbuf[:, columns(g, HEAD_DIM)] = sums[1].astype(jnp.bfloat16)

    @pl.loop(0, last)
    def _(c):
        total_up(c)

    @pl.when(relays)
    def _():
        relay().wait_send()

    @pl.when(passes)
    def _():
        pass_copy.wait_send()

    for k in range(1, back + 1):
        short = edge if k == 1 else jnp.bool_(False)

        @pl.when((me + k < total) & jnp.logical_not(short))
        def _():
            wait_for(window.at[0], kv_send.at[k - 1])

        @pl.when(short)
        def _():
            wait_for(window.at[0, pl.ds(0, last * per)], kv_send.at[k - 1])

        @pl.when(me - k >= 0)
        def _():
            wait_for(part.at[k - 1], g_send.at[k - 1])

    total_up(last)


def write_out(att, dq, dk, dv, att_hbm, dq_hbm, dk_hbm, dv_hbm, sems):
    pairs = ((att, att_hbm), (dq, dq_hbm), (dk, dk_hbm), (dv, dv_hbm))
    copies = [
        pltpu.make_async_copy(source, target, sems.at[which])
        for which, (source, target) in enumerate(pairs)
    ]
    for copy in copies:
        copy.start()
    for copy in copies:
        copy.wait()


def solution(mesh):
    back = mesh.shape["head"]
    total = mesh.shape["blk"] * back

    def per_device(query, key, value, grad_out, doc_lengths):
        rows, kv_heads = query.shape[0], key.shape[1] // HEAD_DIM
        chunks = kv_heads // math.gcd(kv_heads, HEADS_A_COPY)
        bf, f32 = jnp.bfloat16, jnp.float32
        anywhere = pl.BlockSpec(memory_space=pl.ANY)
        dma = pltpu.SemaphoreType.DMA
        results = pl.pallas_call(
            functools.partial(kernel, back, total),
            out_shape=[
                pltpu.VMEM(query.shape, bf),
                pltpu.VMEM(query.shape, bf),
                pltpu.VMEM(key.shape, bf),
                pltpu.VMEM(key.shape, bf),
            ],
            in_specs=[anywhere] * 5,
            out_specs=[pl.BlockSpec(memory_space=pltpu.VMEM)] * 4,
            scratch_shapes=[
                pltpu.VMEM((back + 1, kv_heads, 2, rows, HEAD_DIM), bf),
                pltpu.VMEM((2, *query.shape), bf),
                pltpu.VMEM((back, kv_heads, 2, rows, HEAD_DIM), bf),
                pltpu.VMEM((back, kv_heads, 2, rows, HEAD_DIM), bf),
                pltpu.VMEM((kv_heads // chunks, 2, rows, HEAD_DIM), bf),
                pltpu.VMEM((kv_heads, 2, rows, HEAD_DIM), f32),
                pltpu.VMEM(((back + 1) * rows, rows), f32),
                pltpu.SMEM(doc_lengths.shape, jnp.int32),
                dma,
                dma,
                dma((back,)),
                dma((chunks,)),
                dma,
                dma,
                dma((back,)),
                dma((chunks,)),
            ],
            compiler_params=pltpu.CompilerParams(collective_id=0, has_side_effects=True),
        )(doc_lengths, query, key, value, grad_out)
        results = [pltpu.with_memory_space_constraint(r, pltpu.VMEM) for r in results]
        return pl.pallas_call(
            write_out,
            out_shape=[
                jax.ShapeDtypeStruct(query.shape, bf),
                jax.ShapeDtypeStruct(query.shape, bf),
                jax.ShapeDtypeStruct(key.shape, bf),
                jax.ShapeDtypeStruct(key.shape, bf),
            ],
            in_specs=[pl.BlockSpec(memory_space=pltpu.VMEM)] * 4,
            out_specs=[anywhere] * 4,
            scratch_shapes=[dma((4,))],
        )(*results)

    split = P(("blk", "head"), None)
    return jax.shard_map(
        per_device,
        mesh=mesh,
        in_specs=(split, split, split, split, P()),
        out_specs=(split, split, split, split),
        check_vma=False,
    )
```

```python
import functools
import math

import jax
import jax.numpy as jnp
from jax import lax
from jax.experimental import pallas as pl
from jax.experimental.pallas import tpu as pltpu
from jax.sharding import PartitionSpec as P

HEAD_DIM = 128
EXCLUDED = -1e30
HEADS_A_COPY = 2
MESH = pl.DeviceIdType.MESH


def kernel(
    back, total, lens_hbm, q_hbm, k_hbm, v_hbm, do_hbm, attbuf, dqbuf, dkbuf, dvbuf,
    window, qbuf, part, landed, passing, own, bias, lens,
    lens_in, kv_in, kv_send, kv_recv, detour_recv, detour_send, g_send, g_recv,
):
    rows = q_hbm.shape[0]
    kv_heads = k_hbm.shape[1] // HEAD_DIM
    groups = q_hbm.shape[1] // k_hbm.shape[1]
    span = (back + 1) * rows
    scaling = HEAD_DIM ** (-0.5)
    chunks = g_recv.shape[0]
    per = kv_heads // chunks
    last = chunks - 1
    me = lax.axis_index("blk") * back + lax.axis_index("head")
    place = me % (2 * back)
    edge = (place == 2 * back - 1) & (me + back < total) & (back == 2)
    relays = (place == 1) & (me > back) & (back == 2)
    around = (place == 0) & (me > back) & (back == 2)
    passes = (place == 2) & (me + back < total) & (back == 2)

    def device(number):
        return {"blk": number // back, "head": number % back}

    def columns(g, size):
        return pl.ds(pl.multiple_of(g * size, size), size)

    def heads(c):
        return pl.ds(c * per, per)

    def kv_load(g, which):
        return pltpu.make_async_copy(
            (k_hbm, v_hbm)[which].at[:, columns(g, HEAD_DIM)],
            window.at[0, g, which],
            kv_in,
        )

    q_load = pltpu.make_async_copy(q_hbm, qbuf.at[0], kv_in)
    do_load = pltpu.make_async_copy(do_hbm, qbuf.at[1], kv_in)

    def wait_for(landing, sem):
        pltpu.make_async_copy(landing, landing, sem).wait()

    def kv_copy(c, k):
        return pltpu.make_async_remote_copy(
            src_ref=window.at[0, heads(c)],
            dst_ref=window.at[k, heads(c)],
            send_sem=kv_send.at[k - 1],
            recv_sem=kv_recv.at[c],
            device_id=device(me + k),
            device_id_type=MESH,
        )

    def first_copy(g, which, k):
        return pltpu.make_async_remote_copy(
            src_ref=(k_hbm, v_hbm)[which].at[:, columns(g, HEAD_DIM)],
            dst_ref=window.at[k, g, which],
            send_sem=kv_send.at[k - 1],
            recv_sem=kv_recv.at[0],
            device_id=device(me + k),
            device_id_type=MESH,
        )

    edge_copy = pltpu.make_async_remote_copy(
        src_ref=window.at[0, heads(last)],
        dst_ref=window.at[back, heads(last)],
        send_sem=kv_send.at[back - 1],
        recv_sem=detour_recv,
        device_id=device(me + back),
        device_id_type=MESH,
    )

    def relay():
        return pltpu.make_async_remote_copy(
            src_ref=window.at[back, heads(last)],
            dst_ref=window.at[1, heads(last)],
            send_sem=detour_send,
            recv_sem=kv_recv.at[last],
            device_id=device(me - 1),
            device_id_type=MESH,
        )

    def g_copy(g, k):
        return pltpu.make_async_remote_copy(
            src_ref=part.at[k - 1, g],
            dst_ref=landed.at[k - 1, g],
            send_sem=g_send.at[k - 1],
            recv_sem=g_recv.at[g // per],
            device_id=device(me - k),
            device_id_type=MESH,
        )

    barrier = pltpu.get_barrier_semaphore()
    for k in range(1, back + 1):
        @pl.when(me - k >= 0)
        def _():
            pl.semaphore_signal(barrier, inc=1, device_id=device(me - k), device_id_type=MESH)

    around_copy = pltpu.make_async_remote_copy(
        src_ref=part.at[0, heads(0)],
        dst_ref=passing,
        send_sem=g_send.at[0],
        recv_sem=detour_recv,
        device_id=device(me - back),
        device_id_type=MESH,
    )
    pass_copy = pltpu.make_async_remote_copy(
        src_ref=passing,
        dst_ref=landed.at[0, heads(0)],
        send_sem=detour_send,
        recv_sem=g_recv.at[0],
        device_id=device(me + 1),
        device_id_type=MESH,
    )

    eager = place == 1

    def load():
        @pl.loop(0, kv_heads)
        def _(g):
            kv_load(g, 0).start()
            kv_load(g, 1).start()

    @pl.when(jnp.logical_not(eager))
    def _():
        load()

    @pl.when(me < total - 1)
    def _():
        pl.semaphore_wait(barrier, jnp.minimum(total - 1 - me, back))

    @pl.when(eager)
    def _():
        for g in range(per):
            for which in range(2):
                first_copy(g, which, 1).start()

        load()

    lens_load = pltpu.make_async_copy(lens_hbm, lens, lens_in)
    lens_load.start()
    wait_for(window.at[0], kv_in)

    @pl.when(edge)
    def _():
        kv_copy(0, 1).start()
        edge_copy.start()
        kv_copy(0, back).start()

    @pl.loop(edge.astype(jnp.int32), chunks - edge.astype(jnp.int32))
    def _(c):
        for k in range(1, back + 1):
            later = (relays & (c == last)) | (eager & (c == 0)) if k == 1 else False
            @pl.when((me + k < total) & jnp.logical_not(later))
            def _():
                kv_copy(c, k).start()


    for k in range(1, back + 1):
        @pl.when(me - k < 0)
        def _():
            window[k] = jnp.zeros((kv_heads, 2, rows, HEAD_DIM), jnp.bfloat16)

        @pl.when(me + k >= total)
        def _():
            landed[k - 1] = jnp.zeros((kv_heads, 2, rows, HEAD_DIM), jnp.bfloat16)

    q_load.start()
    do_load.start()
    lens_load.wait()
    query_pos = me * rows + lax.broadcasted_iota(jnp.int32, (1, rows), 1)

    def latest(d, carry):
        start, first = carry
        return start + lens[d], jnp.where(query_pos >= start, start, first)

    _, first = lax.fori_loop(
        0, lens.shape[0], latest, (jnp.int32(0), jnp.zeros((1, rows), jnp.int32))
    )
    key_pos = (me - back) * rows + lax.broadcasted_iota(jnp.int32, (span, rows), 0)
    bias[...] = jnp.where((key_pos <= query_pos) & (key_pos >= first), 0.0, EXCLUDED)

    def dot(a, b, a_dim, b_dim):
        return lax.dot_general(
            a, b, (((a_dim,), (b_dim,)), ((), ())), preferred_element_type=jnp.float32
        )

    def stacked(which, g):
        return jnp.concatenate(
            [qbuf[which, :, columns(g * groups + h, HEAD_DIM)] for h in range(groups)], axis=0
        )

    wait_for(qbuf, kv_in)

    @pl.loop(0, kv_heads)
    def _(g):
        @pl.when(g % per == 0)
        def _():
            early = relays & (g == last * per)
            for n in range(1, back + 1):
                @pl.when((jnp.minimum(me, back) - early.astype(jnp.int32)) == n)
                def _():
                    wait_for(window.at[pl.ds(1, n), heads(g // per)], kv_recv.at[g // per])

        @pl.when(relays & (g == 0))
        def _():
            edge_copy.wait_recv()
            relay().start()
            kv_copy(last, 1).start()

        @pl.when(passes & (g == kv_heads - 1))
        def _():
            around_copy.wait_recv()
            pass_copy.start()

        keys, values = (
            jnp.concatenate([window[k, g, which] for k in range(back, -1, -1)], axis=0)
            for which in range(2)
        )
        queries, grads = stacked(0, g), stacked(1, g)
        kept = jnp.concatenate([bias[...]] * groups, axis=1)
        scores = dot(keys, queries, 1, 1) * (scaling * math.log2(math.e)) + kept
        peak = jnp.max(scores, axis=0, keepdims=True)
        raised = jnp.exp2(scores - peak)
        weights = raised * (1.0 / jnp.sum(raised, axis=0, keepdims=True))
        weights_bf = weights.astype(jnp.bfloat16)
        attended = dot(values, weights_bf, 0, 0)
        grad_weights = dot(values, grads, 1, 1)
        delta = jnp.sum(weights * grad_weights, axis=0, keepdims=True)
        grad_scores = (weights * (grad_weights - delta)).astype(jnp.bfloat16)
        grad_query = dot(keys, grad_scores, 0, 0) * scaling
        grad_key = dot(grad_scores, queries, 1, 0) * scaling
        grad_value = dot(weights_bf, grads, 1, 0)
        for k in range(1, back + 1):
            at = slice((back - k) * rows, (back - k + 1) * rows)
            part[k - 1, g, 0] = grad_key[at].astype(jnp.bfloat16)
            part[k - 1, g, 1] = grad_value[at].astype(jnp.bfloat16)
        own[g, 0] = grad_key[back * rows :]
        own[g, 1] = grad_value[back * rows :]

        @pl.when(around & (g == per - 1))
        def _():
            around_copy.start()

        for k in range(back, 0, -1):
            detour = around & (g < per) if k == 1 else False
            @pl.when((me - k >= 0) & jnp.logical_not(detour))
            def _():
                g_copy(g, k).start()

        for h in range(groups):
            at = slice(h * HEAD_DIM, (h + 1) * HEAD_DIM)
            to = columns(g * groups + h, HEAD_DIM)
            attbuf[:, to] = attended[:, at].T.astype(jnp.bfloat16)
            dqbuf[:, to] = grad_query[:, at].T.astype(jnp.bfloat16)

    def total_up(c):
        for n in range(1, back + 1):
            @pl.when(jnp.minimum(total - 1 - me, back) == n)
            def _():
                wait_for(landed.at[pl.ds(0, n), heads(c)], g_recv.at[c])

        for i in range(per):
            g = c * per + i
            sums = own[g]
            for k in range(1, back + 1):
                sums = sums + landed[k - 1, g].astype(jnp.float32)
            dkbuf[:, columns(g, HEAD_DIM)] = sums[0].astype(jnp.bfloat16)
            dvbuf[:, columns(g, HEAD_DIM)] = sums[1].astype(jnp.bfloat16)

    @pl.loop(0, last)
    def _(c):
        total_up(c)

    @pl.when(relays)
    def _():
        relay().wait_send()

    @pl.when(passes)
    def _():
        pass_copy.wait_send()

    for k in range(1, back + 1):
        short = edge if k == 1 else jnp.bool_(False)

        @pl.when((me + k < total) & jnp.logical_not(short))
        def _():
            wait_for(window.at[0], kv_send.at[k - 1])

        @pl.when(short)
        def _():
            wait_for(window.at[0, pl.ds(0, last * per)], kv_send.at[k - 1])

        @pl.when(me - k >= 0)
        def _():
            wait_for(part.at[k - 1], g_send.at[k - 1])

    total_up(last)


def write_out(att, dq, dk, dv, att_hbm, dq_hbm, dk_hbm, dv_hbm, sems):
    pairs = ((att, att_hbm), (dq, dq_hbm), (dk, dk_hbm), (dv, dv_hbm))
    copies = [
        pltpu.make_async_copy(source, target, sems.at[which])
        for which, (source, target) in enumerate(pairs)
    ]
    for copy in copies:
        copy.start()
    for copy in copies:
        copy.wait()


def solution(mesh):
    back = mesh.shape["head"]
    total = mesh.shape["blk"] * back

    def per_device(query, key, value, grad_out, doc_lengths):
        rows, kv_heads = query.shape[0], key.shape[1] // HEAD_DIM
        chunks = kv_heads // math.gcd(kv_heads, HEADS_A_COPY)
        bf, f32 = jnp.bfloat16, jnp.float32
        anywhere = pl.BlockSpec(memory_space=pl.ANY)
        dma = pltpu.SemaphoreType.DMA
        results = pl.pallas_call(
            functools.partial(kernel, back, total),
            out_shape=[
                pltpu.VMEM(query.shape, bf),
                pltpu.VMEM(query.shape, bf),
                pltpu.VMEM(key.shape, bf),
                pltpu.VMEM(key.shape, bf),
            ],
            in_specs=[anywhere] * 5,
            out_specs=[pl.BlockSpec(memory_space=pltpu.VMEM)] * 4,
            scratch_shapes=[
                pltpu.VMEM((back + 1, kv_heads, 2, rows, HEAD_DIM), bf),
                pltpu.VMEM((2, *query.shape), bf),
                pltpu.VMEM((back, kv_heads, 2, rows, HEAD_DIM), bf),
                pltpu.VMEM((back, kv_heads, 2, rows, HEAD_DIM), bf),
                pltpu.VMEM((kv_heads // chunks, 2, rows, HEAD_DIM), bf),
                pltpu.VMEM((kv_heads, 2, rows, HEAD_DIM), f32),
                pltpu.VMEM(((back + 1) * rows, rows), f32),
                pltpu.SMEM(doc_lengths.shape, jnp.int32),
                dma,
                dma,
                dma((back,)),
                dma((chunks,)),
                dma,
                dma,
                dma((back,)),
                dma((chunks,)),
            ],
            compiler_params=pltpu.CompilerParams(collective_id=0, has_side_effects=True),
        )(doc_lengths, query, key, value, grad_out)
        results = [pltpu.with_memory_space_constraint(r, pltpu.VMEM) for r in results]
        return pl.pallas_call(
            write_out,
            out_shape=[
                jax.ShapeDtypeStruct(query.shape, bf),
                jax.ShapeDtypeStruct(query.shape, bf),
                jax.ShapeDtypeStruct(key.shape, bf),
                jax.ShapeDtypeStruct(key.shape, bf),
            ],
            in_specs=[pl.BlockSpec(memory_space=pltpu.VMEM)] * 4,
            out_specs=[anywhere] * 4,
            scratch_shapes=[dma((4,))],
        )(*results)

    split = P(("blk", "head"), None)
    return jax.shard_map(
        per_device,
        mesh=mesh,
        in_specs=(split, split, split, split, P()),
        out_specs=(split, split, split, split),
        check_vma=False,
    )
```
